16 devices in a mesh: pp: 2 (over z), dp: 8 (over y, x, core).
Axes of the slice: x: 2, y: 2, z: 2, core: 2. Of those that a mesh axis runs over, the one named last changes fastest.
Arguments:
- tok_ids: int32 [2, 4096], P(None, 'dp')
- d_out: bfloat16 [2, 4096, 128], P('pp', 'dp')
- stored_x: bfloat16 [2, 2, 4096, 128], P('pp', None, 'dp')
- w_in: bfloat16 [24, 128, 512], P('pp')
- w_out: bfloat16 [24, 512, 128], P('pp')
- acc_in: float32 [24, 8, 128, 512], P('pp', 'dp')
- acc_out: float32 [24, 8, 512, 128], P('pp', 'dp')
- acc_emb: float32 [8, 30522, 128], P('dp')
Outputs:
- output 1: float32 [24, 128, 512], P('pp', 'dp')
- output 2: float32 [24, 512, 128], P('pp', 'dp')
- output 3: float32 [30522, 128], P(None, 'dp')
All inputs are finite; a program needn't handle non-finite values.
Results may differ from the reference program's by a relative error of at most 0.0176994.
Values are sent between devices in bfloat16 or wider.
A program may use at most 1 GiB of HBM per device.

```python
import jax
import jax.numpy as jnp
from jax import lax

STAGES = 2
REPLICAS = 8
LAYERS = 12
HID = 128
FF = 512
VOCAB = 30522
TOKENS_DEV = 512

ROWS_ALL = TOKENS_DEV * REPLICAS


def setup_inputs(seed: int = 0) -> dict:
    key_list = jax.random.split(jax.random.key(seed), 8)
    tok_ids = jax.random.randint(key_list[0], (STAGES, ROWS_ALL), 0, VOCAB, dtype=jnp.int32)
    d_out = jax.random.normal(key_list[1], (STAGES, ROWS_ALL, HID), jnp.float32).astype(jnp.bfloat16)
    stored_x = jax.random.normal(key_list[2], (STAGES, STAGES, ROWS_ALL, HID), jnp.float32).astype(jnp.bfloat16)
    w_in = (jax.random.normal(key_list[3], (STAGES * LAYERS, HID, FF), jnp.float32) * HID ** -0.5).astype(jnp.bfloat16)
    w_out = (jax.random.normal(key_list[4], (STAGES * LAYERS, FF, HID), jnp.float32) * (FF * STAGES * LAYERS) ** -0.5).astype(jnp.bfloat16)
    in_scale = 0.2 * (TOKENS_DEV / LAYERS) ** 0.5
    out_scale = 0.4 * (TOKENS_DEV * STAGES) ** 0.5
    acc_in = jax.random.normal(key_list[5], (STAGES * LAYERS, REPLICAS, HID, FF), jnp.float32) * in_scale
    acc_out = jax.random.normal(key_list[6], (STAGES * LAYERS, REPLICAS, FF, HID), jnp.float32) * out_scale
    acc_emb = jax.random.normal(key_list[7], (REPLICAS, VOCAB, HID), jnp.float32) * 0.5
    return {'tok_ids': tok_ids, 'd_out': d_out, 'stored_x': stored_x, 'w_in': w_in, 'w_out': w_out, 'acc_in': acc_in, 'acc_out': acc_out, 'acc_emb': acc_emb}


def layer_forward(x_cur, w_in_l, w_out_l):
    pre_act = jnp.dot(x_cur, w_in_l, preferred_element_type=jnp.float32).astype(jnp.bfloat16)
    hidden = jax.nn.gelu(pre_act.astype(jnp.float32)).astype(jnp.bfloat16)
    out_x = (x_cur.astype(jnp.float32) + jnp.dot(hidden, w_out_l, preferred_element_type=jnp.float32)).astype(jnp.bfloat16)
    return out_x, pre_act, hidden


def per_replica(left_rows, right_rows):
    left_r = left_rows.reshape(REPLICAS, TOKENS_DEV, left_rows.shape[-1]).astype(jnp.float32)
    right_r = right_rows.reshape(REPLICAS, TOKENS_DEV, right_rows.shape[-1]).astype(jnp.float32)
    return jnp.einsum('rti,rtf->rif', left_r, right_r)


def stage_backward(w_in_s, w_out_s, acc_in_s, acc_out_s, x_stage, cot_stage):
    def one_micro(carry, item):
        sum_in, sum_out = carry
        x_first, cot_first = item

        def fwd_step(x_cur, weights):
            out_x, pre_act, hidden = layer_forward(x_cur, weights[0], weights[1])
            return out_x, (x_cur, pre_act, hidden)

        _, saved_acts = lax.scan(fwd_step, x_first, (w_in_s, w_out_s))

        def bwd_step(cot_cur, layer_item):
            w_in_l, w_out_l, x_cur, pre_act, hidden = layer_item
            g_out = per_replica(hidden, cot_cur)
            d_hidden = jnp.dot(cot_cur, w_out_l.T, preferred_element_type=jnp.float32).astype(jnp.bfloat16)
            pre_f = pre_act.astype(jnp.float32)
            gelu_slope = jax.jvp(jax.nn.gelu, (pre_f,), (jnp.ones_like(pre_f),))[1]
            d_pre = (d_hidden.astype(jnp.float32) * gelu_slope).astype(jnp.bfloat16)
            g_in = per_replica(x_cur, d_pre)
            d_x = (cot_cur.astype(jnp.float32) + jnp.dot(d_pre, w_in_l.T, preferred_element_type=jnp.float32)).astype(jnp.bfloat16)
            return d_x, (g_in, g_out)

        d_first, grads = lax.scan(bwd_step, cot_first, (w_in_s, w_out_s) + saved_acts, reverse=True)
        return (sum_in + grads[0], sum_out + grads[1]), d_first

    sums, d_cots = lax.scan(one_micro, (acc_in_s, acc_out_s), (x_stage, cot_stage))
    return sums[0], sums[1], d_cots


def replica_mean(total, axis_pos):
    return jnp.sum(total.astype(jnp.bfloat16).astype(jnp.float32), axis=axis_pos) / REPLICAS


def reference(tok_ids, d_out, stored_x, w_in, w_out, acc_in, acc_out, acc_emb):
    grads_in = []
    grads_out = []
    cot_rows = d_out[:0]
    for stage_id in range(STAGES - 1, -1, -1):
        pending = STAGES - stage_id
        first_row = stage_id * LAYERS
        last_row = first_row + LAYERS
        cot_rows = jnp.concatenate([cot_rows, d_out[stage_id:stage_id + 1]], axis=0)
        sum_in, sum_out, cot_rows = stage_backward(w_in[first_row:last_row], w_out[first_row:last_row], acc_in[first_row:last_row], acc_out[first_row:last_row], stored_x[stage_id, :pending], cot_rows)
        grads_in = [replica_mean(sum_in, 1)] + grads_in
        grads_out = [replica_mean(sum_out, 1)] + grads_out
    row_replica = jnp.arange(ROWS_ALL, dtype=jnp.int32) // TOKENS_DEV
    segment_ids = (tok_ids + row_replica[None, :] * VOCAB).reshape(-1)
    emb_new = jax.ops.segment_sum(cot_rows.reshape(-1, HID).astype(jnp.float32), segment_ids, num_segments=REPLICAS * VOCAB)
    grad_emb = replica_mean(acc_emb + emb_new.reshape(REPLICAS, VOCAB, HID), 0)
    return (jnp.concatenate(grads_in, axis=0), jnp.concatenate(grads_out, axis=0), grad_emb)
```

```python
import functools

import jax
import jax.numpy as jnp
from jax import lax
from jax.experimental import pallas as pl
from jax.experimental.pallas import tpu as pltpu
from jax.sharding import PartitionSpec as P

MESH = pl.DeviceIdType.MESH
C0 = 0.7978845608028654
C1 = 0.044715
F32, BF16 = jnp.float32, jnp.bfloat16
ANY = pl.BlockSpec(memory_space=pl.ANY)
VM = pl.BlockSpec(memory_space=pltpu.VMEM)


def coords():
    pp, d = lax.axis_index("pp"), lax.axis_index("dp")
    y, x, c = d // 4, (d // 2) % 2, d % 2
    to_x = {"pp": pp, "dp": d + 2 - 4 * x}
    to_y = {"pp": pp, "dp": d + 4 - 8 * y}
    to_c = {"pp": pp, "dp": d + 1 - 2 * c}
    to_z = {"pp": 1 - pp, "dp": d}
    return pp, y, x, c, to_x, to_y, to_c, to_z


def enter(neighbours):
    barrier = pltpu.get_barrier_semaphore()
    for dev in neighbours:
        pl.semaphore_signal(barrier, inc=1, device_id=dev, device_id_type=MESH)
    pl.semaphore_wait(barrier, len(neighbours))


def remote(src, dst, send, recv, dev):
    return pltpu.make_async_remote_copy(src_ref=src, dst_ref=dst, send_sem=send, recv_sem=recv, device_id=dev, device_id_type=MESH)


def slab_xy(d):
    return (d % 2) * 4 + ((d // 2) % 2) * 2 + d // 4


def slab_yx(d):
    return (d % 2) * 4 + (d // 4) * 2 + (d // 2) % 2


class Reduce:
    def __init__(self, src, r0, r1, r2, sems, to, c, p, q):
        self.src, self.r0, self.r1, self.r2, self.sems, self.to = src, r0, r1, r2, sems, to
        self.c, self.p, self.q = c, p, q

    def copy0(self, i):
        return remote(self.src.at[i, pl.ds(4 * (1 - self.c), 4)], self.r0.at[i], self.sems.at[0, i], self.sems.at[1, i], self.to[0])

    def copy1(self, i):
        at = 4 * self.c + 2 * (1 - self.p)
        return remote(self.src.at[i, pl.ds(at, 2)], self.r1.at[i], self.sems.at[2, i], self.sems.at[3, i], self.to[1])

    def copy2(self, i):
        at = 4 * self.c + 2 * self.p + 1 - self.q
        return remote(self.src.at[i, at], self.r2.at[i], self.sems.at[4, i], self.sems.at[5, i], self.to[2])

    def add0(self, i):
        self.copy0(i).wait_recv()
        for k in range(4):
            at = 4 * self.c + k
            self.src[i, at] = (self.src[i, at].astype(F32) + self.r0[i, k].astype(F32)).astype(BF16)

    def add1(self, i):
        self.copy1(i).wait_recv()
        for k in range(2):
            at = 4 * self.c + 2 * self.p + k
            self.src[i, at] = (self.src[i, at].astype(F32) + self.r1[i, k].astype(F32)).astype(BF16)

    def last(self, i):
        self.copy2(i).wait_recv()
        at = 4 * self.c + 2 * self.p + self.q
        return self.src[i, at].astype(F32) + self.r2[i].astype(F32)

    def drain(self, i):
        self.copy0(i).wait_send()
        self.copy1(i).wait_send()
        self.copy2(i).wait_send()


def dot(a, b, ca, cb):
    return lax.dot_general(a, b, (((ca,), (cb,)), ((), ())), preferred_element_type=F32)


def mlp_kernel(layers, chunks, d_out, x_in, w_in, w_out, acc_in, acc_out, g_in, g_out, dx_out,
               w1, w2, xs, hid, slope, gs, dh, dw1, dw2, acc2, cot_in, dxs,
               s1, s1a, s1b, s1c, s2, s2a, s2b, s2c, wsem, asem, zsem, sem1, sem2):
    pp, y, x, c, to_x, to_y, to_c, to_z = coords()
    tokens = d_out.shape[1]
    rows = tokens // chunks

    def load(i):
        return (pltpu.make_async_copy(w_in.at[i], w1.at[i], wsem.at[0, i]),
                pltpu.make_async_copy(w_out.at[i], w2.at[i], wsem.at[1, i]))

    load_acc1 = pltpu.make_async_copy(acc_in.at[:, 0], dw1, asem.at[0])
    load_acc2 = pltpu.make_async_copy(acc_out.at[:, 0], acc2, asem.at[1])
    for i in range(layers):
        for cp in load(i):
            cp.start()
    load_acc1.start()
    load_acc2.start()
    enter((to_x, to_y, to_c, to_z))

    red1 = Reduce(s1, s1a, s1b, s1c, sem1, (to_c, to_x, to_y), c, x, y)
    red2 = Reduce(s2, s2a, s2b, s2c, sem2, (to_c, to_y, to_x), c, y, x)

    def forward(micro, fresh):
        xs[0] = x_in[0, micro]

        def body(i, carry):
            if fresh:
                for cp in load(i):
                    cp.wait()
            for k in range(chunks):
                r = pl.ds(k * rows, rows)
                xc = xs[i, r]
                h = dot(xc, w1[i], 1, 0).astype(BF16).astype(F32)
                h2 = h * h
                t = jnp.tanh(h * (C0 + (C0 * C1) * h2))
                cdf = 0.5 + 0.5 * t
                a = (h * cdf).astype(BF16)
                hid[i, r] = a
                slope[i, r] = cdf + (0.5 * h) * ((1.0 - t * t) * (C0 + (3.0 * C0 * C1) * h2))
                xs[i + 1, r] = (xc.astype(F32) + dot(a, w2[i], 1, 0)).astype(BF16)
            return carry

        lax.fori_loop(0, layers, body, 0)

    def backward(first, final):
        def block(i):
            for k in range(chunks):
                r = pl.ds(k * rows, rows)
                gc = gs[i + 1, r]
                da = dot(gc, w2[i], 1, 1).astype(BF16).astype(F32)
                dhc = (da * slope[i, r]).astype(BF16)
                dh[r] = dhc
                gs[i, r] = (gc.astype(F32) + dot(dhc, w1[i], 1, 1)).astype(BF16)
            new2 = dot(gs[i + 1], hid[i], 0, 0)
            if not first:
                new2 = new2 + dw2[i]
            new1 = dot(xs[i], dh[...], 0, 0) + dw1[i]
            if not final:
                dw1[i] = new1
                dw2[i] = new2
                return
            new1 = new1.astype(BF16)
            n1 = new1.shape[0] // 8
            for d in range(8):
                s1[i, slab_xy(d)] = new1[d * n1:(d + 1) * n1]
            new2 = (new2.T + acc2[i]).astype(BF16)
            n2 = new2.shape[0] // 8
            for d in range(8):
                s2[i, slab_yx(d)] = new2[d * n2:(d + 1) * n2]

        if not final:
            lax.fori_loop(0, layers, lambda k, carry: (block(layers - 1 - k), carry)[1], 0)
            return

        def stage(k, lag, fn):
            @pl.when((k >= lag) & (k < layers + lag))
            def _():
                fn(layers - 1 - (k - lag))

        def step(k, carry):
            stage(k, 1, lambda i: (red1.copy0(i).start(), red2.copy0(i).start()))
            stage(k, 3, lambda i: (red1.copy1(i).start(), red2.copy1(i).start()))
            stage(k, 6, lambda i: (red1.copy2(i).start(), red2.copy2(i).start()))
            stage(k, 0, block)
            stage(k, 2, lambda i: (red1.add0(i), red2.add0(i)))
            stage(k, 5, lambda i: (red1.add1(i), red2.add1(i)))

            def finish(i):
                g_in[i] = red1.last(i) * 0.125
                g_out[i] = red2.last(i) * 0.125

            stage(k, 8, finish)
            return carry

        lax.fori_loop(0, layers + 9, step, 0)

    send_cot = remote(gs.at[0], cot_in, zsem.at[0], zsem.at[1], to_z)
    send_dx1 = remote(dxs.at[1], dxs.at[1], zsem.at[2], zsem.at[3], to_z)
    send_dx0 = remote(dxs.at[0], dxs.at[0], zsem.at[4], zsem.at[5], to_z)

    @pl.when(pp == 1)
    def _():
        forward(0, True)
        load_acc1.wait()
        load_acc2.wait()
        gs[layers] = d_out[0]
        backward(True, True)
        send_cot.start()
        send_cot.wait_send()
        send_dx1.wait_recv()
        send_dx0.wait_recv()

    @pl.when(pp == 0)
    def _():
        forward(1, True)
        load_acc1.wait()
        load_acc2.wait()
        gs[layers] = d_out[0]
        backward(True, False)
        dxs[1] = gs[0]
        send_dx1.start()
        forward(0, False)
        send_cot.wait_recv()
        gs[layers] = cot_in[...]
        backward(False, True)
        dxs[0] = gs[0]
        send_dx0.start()
        send_dx1.wait_send()
        send_dx0.wait_send()

    dx_out[...] = dxs[...]

    def drain(i, carry):
        red1.drain(i)
        red2.drain(i)
        return carry

    lax.fori_loop(0, layers, drain, 0)


def mlp(d_out, stored_x, w_in, w_out, acc_in, acc_out):
    layers, hid, ff = w_in.shape
    tokens = d_out.shape[1]
    n1, n2 = hid // 8, ff // 8
    return pl.pallas_call(
        functools.partial(mlp_kernel, layers, 4),
        out_shape=(jax.ShapeDtypeStruct((layers, n1, ff), F32), jax.ShapeDtypeStruct((layers, n2, hid), F32),
                   jax.ShapeDtypeStruct((2, tokens, hid), BF16)),
        in_specs=[VM, VM, ANY, ANY, ANY, ANY],
        out_specs=(VM, VM, VM),
        scratch_shapes=[
            pltpu.VMEM((layers, hid, ff), BF16),
            pltpu.VMEM((layers, ff, hid), BF16),
            pltpu.VMEM((layers + 1, tokens, hid), BF16),
            pltpu.VMEM((layers, tokens, ff), BF16),
            pltpu.VMEM((layers, tokens, ff), F32),
            pltpu.VMEM((layers + 1, tokens, hid), BF16),
            pltpu.VMEM((tokens, ff), BF16),
            pltpu.VMEM((layers, hid, ff), F32),
            pltpu.VMEM((layers, hid, ff), F32),
            pltpu.VMEM((layers, ff, hid), F32),
            pltpu.VMEM((tokens, hid), BF16),
            pltpu.VMEM((2, tokens, hid), BF16),
            pltpu.VMEM((layers, 8, n1, ff), BF16),
            pltpu.VMEM((layers, 4, n1, ff), BF16),
            pltpu.VMEM((layers, 2, n1, ff), BF16),
            pltpu.VMEM((layers, n1, ff), BF16),
            pltpu.VMEM((layers, 8, n2, hid), BF16),
            pltpu.VMEM((layers, 4, n2, hid), BF16),
            pltpu.VMEM((layers, 2, n2, hid), BF16),
            pltpu.VMEM((layers, n2, hid), BF16),
            pltpu.SemaphoreType.DMA((2, layers)),
            pltpu.SemaphoreType.DMA((2,)),
            pltpu.SemaphoreType.DMA((6,)),
            pltpu.SemaphoreType.DMA((6, layers)),
            pltpu.SemaphoreType.DMA((6, layers)),
        ],
        compiler_params=pltpu.CompilerParams(collective_id=0, has_side_effects=True, vmem_limit_bytes=63 * 2**20),
    )(d_out, stored_x, w_in, w_out, acc_in, acc_out)


def emb_kernel(pairs, width, rel_ids, dx, acc, out, buf, dxt, sa, sa0, sa1, sa2, sb, sb0, sb1, sb2, fa, fb, za, zb,
               asem, sema, semb, zsem):
    pp, y, x, c, to_x, to_y, to_c, to_z = coords()
    half = 2 * pairs * width
    vocab = acc.shape[0]
    block = 256

    def load(p, size, base):
        return pltpu.make_async_copy(acc.at[pl.ds(base + p * 2 * width, size), 0, :], buf.at[pl.ds(p * 2 * width, size)], asem.at[p])

    def each_load(act):
        for p in range(pairs):
            tail = vocab - half - p * 2 * width
            @pl.when(pp == 0)
            def _():
                act(load(p, 2 * width, 0))

            if tail > 0:
                @pl.when(pp == 1)
                def _():
                    act(load(p, min(2 * width, tail), half))

    each_load(lambda cp: cp.start())
    enter((to_x, to_y, to_c, to_z))
    dxt[...] = dx[...].T
    each_load(lambda cp: cp.wait())

    reda = Reduce(sa, sa0, sa1, sa2, sema, (to_c, to_x, to_y), c, x, y)
    redb = Reduce(sb, sb0, sb1, sb2, semb, (to_c, to_y, to_x), c, y, x)

    def zcopy(i):
        return (remote(fa.at[i], za.at[i], zsem.at[0, i], zsem.at[1, i], to_z),
                remote(fb.at[i], zb.at[i], zsem.at[2, i], zsem.at[3, i], to_z))

    def build(i):
        for part, dst, slab in ((0, sa, slab_xy), (1, sb, slab_yx)):
            def piece(j, carry):
                at = pl.multiple_of(j * block, block)
                row = pl.multiple_of((2 * i + part) * width + j * block, block)
                base = pp * half + row
                ids = rel_ids[...]
                hot = jnp.concatenate([jnp.where(ids == base + 128 * n, 1.0, 0.0).astype(BF16) for n in range(block // 128)], axis=1)
                val = buf[pl.ds(row, block), :].T + dot(dxt[...], hot, 1, 0)
                val = val.astype(BF16)
                for d in range(8):
                    dst[i, slab(d), :, pl.ds(at, block)] = val[d * 16:(d + 1) * 16]
                return carry

            lax.fori_loop(0, width // block, piece, 0)

    def stage(k, lag, fn):
        @pl.when((k >= lag) & (k < pairs + lag))
        def _():
            fn(k - lag)

    def step(k, carry):
        stage(k, 1, lambda i: (reda.copy0(i).start(), redb.copy0(i).start()))
        stage(k, 2, lambda i: (reda.copy1(i).start(), redb.copy1(i).start()))
        stage(k, 4, lambda i: (reda.copy2(i).start(), redb.copy2(i).start()))
        stage(k, 6, lambda i: [cp.start() for cp in zcopy(i)])
        stage(k, 0, build)
        stage(k, 1, lambda i: (reda.add0(i), redb.add0(i)))
        stage(k, 3, lambda i: (reda.add1(i), redb.add1(i)))

        def finish(i):
            fa[i] = reda.last(i).astype(BF16)
            fb[i] = redb.last(i).astype(BF16)

        stage(k, 5, finish)
        return carry

    lax.fori_loop(0, pairs + 7, step, 0)

    def put(i, carry):
        for cp in zcopy(i):
            cp.wait_recv()
        for part, mine, other in ((0, fa, za), (1, fb, zb)):
            off = (2 * i + part) * width
            out[:, pl.ds(pl.multiple_of(pp * half + off, 128), width)] = mine[i]
            out[:, pl.ds(pl.multiple_of((1 - pp) * half + off, 128), width)] = other[i]
        reda.drain(i)
        redb.drain(i)
        for cp in zcopy(i):
            cp.wait_send()
        return carry

    lax.fori_loop(0, pairs, put, 0)


def embed(rel_ids, dx, acc_emb):
    vocab, _, hid = acc_emb.shape
    pairs, width = 6, 1280
    half = 2 * pairs * width
    n = hid // 8
    side = [
        pltpu.VMEM((pairs, 8, n, width), BF16),
        pltpu.VMEM((pairs, 4, n, width), BF16),
        pltpu.VMEM((pairs, 2, n, width), BF16),
        pltpu.VMEM((pairs, n, width), BF16),
    ]
    piece = pltpu.VMEM((pairs, n, width), BF16)
    return pl.pallas_call(
        functools.partial(emb_kernel, pairs, width),
        out_shape=jax.ShapeDtypeStruct((n, 2 * half), BF16),
        in_specs=[VM, VM, ANY],
        out_specs=VM,
        scratch_shapes=[
            pltpu.VMEM((half, hid), F32),
            pltpu.VMEM((hid, dx.shape[0]), BF16),
            *side, *side, piece, piece, piece, piece,
            pltpu.SemaphoreType.DMA((pairs,)),
            pltpu.SemaphoreType.DMA((6, pairs)),
            pltpu.SemaphoreType.DMA((6, pairs)),
            pltpu.SemaphoreType.DMA((4, pairs)),
        ],
        compiler_params=pltpu.CompilerParams(collective_id=1, has_side_effects=True, vmem_limit_bytes=63 * 2**20),
    )(rel_ids, dx, acc_emb)


def solution(mesh):
    def device_body(tok_ids, d_out, stored_x, w_in, w_out, acc_in, acc_out, acc_emb):
        grad_in, grad_out, dx = mlp(d_out, stored_x, w_in, w_out, acc_in, acc_out)
        vocab, hid = acc_emb.shape[1:]
        lane = lax.broadcasted_iota(jnp.int32, (1, 128), 1)
        rel_ids = tok_ids.reshape(-1, 1) - lane
        total = embed(rel_ids, dx.reshape(-1, hid), acc_emb.reshape(vocab, 1, hid))
        grad_emb = total[:, :vocab].T.astype(F32) * 0.125
        return grad_in, grad_out, grad_emb

    return jax.shard_map(
        device_body,
        mesh=mesh,
        in_specs=(P(None, "dp"), P("pp", "dp", None), P("pp", None, "dp", None), P("pp", None, None), P("pp", None, None),
                  P("pp", "dp", None, None), P("pp", "dp", None, None), P("dp", None, None)),
        out_specs=(P("pp", "dp", None), P("pp", "dp", None), P(None, "dp")),
        check_vma=False,
    )
```

```python
import functools

import jax
import jax.numpy as jnp
from jax import lax
from jax.experimental import pallas as pl
from jax.experimental.pallas import tpu as pltpu
from jax.sharding import PartitionSpec as P

MESH = pl.DeviceIdType.MESH
C0 = 0.7978845608028654
C1 = 0.044715
F32, BF16 = jnp.float32, jnp.bfloat16
ANY = pl.BlockSpec(memory_space=pl.ANY)
VM = pl.BlockSpec(memory_space=pltpu.VMEM)


def coords():
    pp, d = lax.axis_index("pp"), lax.axis_index("dp")
    y, x, c = d // 4, (d // 2) % 2, d % 2
    to_x = {"pp": pp, "dp": d + 2 - 4 * x}
    to_y = {"pp": pp, "dp": d + 4 - 8 * y}
    to_c = {"pp": pp, "dp": d + 1 - 2 * c}
    to_z = {"pp": 1 - pp, "dp": d}
    return pp, y, x, c, to_x, to_y, to_c, to_z


def enter(neighbours):
    barrier = pltpu.get_barrier_semaphore()
    for dev in neighbours:
        pl.semaphore_signal(barrier, inc=1, device_id=dev, device_id_type=MESH)
    pl.semaphore_wait(barrier, len(neighbours))


def remote(src, dst, send, recv, dev):
    return pltpu.make_async_remote_copy(src_ref=src, dst_ref=dst, send_sem=send, recv_sem=recv, device_id=dev, device_id_type=MESH)


def slab_xy(d):
    return (d % 2) * 4 + ((d // 2) % 2) * 2 + d // 4


def slab_yx(d):
    return (d % 2) * 4 + (d // 4) * 2 + (d // 2) % 2


class Reduce:
    def __init__(self, src, r0, r1, r2, sems, to, c, p, q):
        self.src, self.r0, self.r1, self.r2, self.sems, self.to = src, r0, r1, r2, sems, to
        self.c, self.p, self.q = c, p, q

    def copy0(self, i):
        return remote(self.src.at[i, pl.ds(4 * (1 - self.c), 4)], self.r0.at[i], self.sems.at[0, i], self.sems.at[1, i], self.to[0])

    def copy1(self, i):
        at = 4 * self.c + 2 * (1 - self.p)
        return remote(self.src.at[i, pl.ds(at, 2)], self.r1.at[i], self.sems.at[2, i], self.sems.at[3, i], self.to[1])

    def copy2(self, i):
        at = 4 * self.c + 2 * self.p + 1 - self.q
        return remote(self.src.at[i, at], self.r2.at[i], self.sems.at[4, i], self.sems.at[5, i], self.to[2])

    def add0(self, i):
        self.copy0(i).wait_recv()
        for k in range(4):
            at = 4 * self.c + k
            self.src[i, at] = (self.src[i, at].astype(F32) + self.r0[i, k].astype(F32)).astype(BF16)

    def add1(self, i):
        self.copy1(i).wait_recv()
        for k in range(2):
            at = 4 * self.c + 2 * self.p + k
            self.src[i, at] = (self.src[i, at].astype(F32) + self.r1[i, k].astype(F32)).astype(BF16)

    def last(self, i):
        self.copy2(i).wait_recv()
        at = 4 * self.c + 2 * self.p + self.q
        return self.src[i, at].astype(F32) + self.r2[i].astype(F32)

    def drain(self, i):
        self.copy0(i).wait_send()
        self.copy1(i).wait_send()
        self.copy2(i).wait_send()


def dot(a, b, ca, cb):
    return lax.dot_general(a, b, (((ca,), (cb,)), ((), ())), preferred_element_type=F32)


def mlp_kernel(layers, chunks, d_out, x_in, w_in, w_out, acc_in, acc_out, g_in, g_out, dx_out,
               w1, w2, xs, hid, slope, gs, dh, dw1, dw2, acc2, cot_in, dxs,
               s1, s1a, s1b, s1c, s2, s2a, s2b, s2c, wsem, asem, zsem, sem1, sem2):
    pp, y, x, c, to_x, to_y, to_c, to_z = coords()
    tokens = d_out.shape[1]
    rows = tokens // chunks

    def load(i):
        return (pltpu.make_async_copy(w_in.at[i], w1.at[i], wsem.at[0, i]),
                pltpu.make_async_copy(w_out.at[i], w2.at[i], wsem.at[1, i]))

    load_acc1 = pltpu.make_async_copy(acc_in.at[:, 0], dw1, asem.at[0])
    load_acc2 = pltpu.make_async_copy(acc_out.at[:, 0], acc2, asem.at[1])
    for i in range(layers):
        for cp in load(i):
            cp.start()
    load_acc1.start()
    load_acc2.start()
    enter((to_x, to_y, to_c, to_z))

    red1 = Reduce(s1, s1a, s1b, s1c, sem1, (to_c, to_x, to_y), c, x, y)
    red2 = Reduce(s2, s2a, s2b, s2c, sem2, (to_c, to_y, to_x), c, y, x)

    def forward(micro, fresh):
        xs[0] = x_in[0, micro]

        def body(i, carry):
            if fresh:
                for cp in load(i):
                    cp.wait()
            for k in range(chunks):
                r = pl.ds(k * rows, rows)
                xc = xs[i, r]
                h = dot(xc, w1[i], 1, 0).astype(BF16).astype(F32)
                h2 = h * h
                t = jnp.tanh(h * (C0 + (C0 * C1) * h2))
                cdf = 0.5 + 0.5 * t
                a = (h * cdf).astype(BF16)
                hid[i, r] = a
                slope[i, r] = cdf + h * ((cdf * (1.0 - cdf)) * (2.0 * C0 + (6.0 * C0 * C1) * h2))
                xs[i + 1, r] = (xc.astype(F32) + dot(a, w2[i], 1, 0)).astype(BF16)
            return carry

        lax.fori_loop(0, layers, body, 0)

    def backward(first, final, send=None):
        def block(i):
            for k in range(chunks):
                r = pl.ds(k * rows, rows)
                gc = gs[i + 1, r]
                da = dot(gc, w2[i], 1, 1).astype(BF16).astype(F32)
                dhc = (da * slope[i, r]).astype(BF16)
                dh[r] = dhc
                gs[i, r] = (gc.astype(F32) + dot(dhc, w1[i], 1, 1)).astype(BF16)
            new2 = dot(gs[i + 1], hid[i], 0, 0)
            if not first:
                new2 = new2 + dw2[i]
            new1 = dot(xs[i], dh[...], 0, 0) + dw1[i]
            if not final:
                dw1[i] = new1
                dw2[i] = new2
                return
            new1 = new1.astype(BF16)
            n1 = new1.shape[0] // 8
            for d in range(8):
                s1[i, slab_xy(d)] = new1[d * n1:(d + 1) * n1]
            new2 = (new2.T + acc2[i]).astype(BF16)
            n2 = new2.shape[0] // 8
            for d in range(8):
                s2[i, slab_yx(d)] = new2[d * n2:(d + 1) * n2]

        if not final:
            lax.fori_loop(0, layers, lambda k, carry: (block(layers - 1 - k), carry)[1], 0)
            return

        def stage(k, lag, fn):
            @pl.when((k >= lag) & (k < layers + lag))
            def _():
                fn(layers - 1 - (k - lag))

        def step(k, carry):
            @pl.when(k == layers)
            def _():
                send.start()

            stage(k, 1, lambda i: (red1.copy0(i).start(), red2.copy0(i).start()))
            stage(k, 3, lambda i: (red1.copy1(i).start(), red2.copy1(i).start()))
            stage(k, 6, lambda i: (red1.copy2(i).start(), red2.copy2(i).start()))
            stage(k, 0, block)
            stage(k, 2, lambda i: (red1.add0(i), red2.add0(i)))
            stage(k, 5, lambda i: (red1.add1(i), red2.add1(i)))

            def finish(i):
                g_in[i] = red1.last(i) * 0.125
                g_out[i] = red2.last(i) * 0.125

            stage(k, 8, finish)
            return carry

        lax.fori_loop(0, layers + 9, step, 0)

    send_cot = remote(gs.at[0], cot_in, zsem.at[0], zsem.at[1], to_z)
    send_dx1 = remote(dxs.at[1], dxs.at[1], zsem.at[2], zsem.at[3], to_z)
    send_dx0 = remote(gs.at[0], dxs.at[0], zsem.at[4], zsem.at[5], to_z)

    @pl.when(pp == 1)
    def _():
        forward(0, True)
        load_acc1.wait()
        load_acc2.wait()
        gs[layers] = d_out[0]
        backward(True, True, send_cot)
        send_cot.wait_send()
        send_dx1.wait_recv()
        send_dx0.wait_recv()

    @pl.when(pp == 0)
    def _():
        forward(1, True)
        load_acc1.wait()
        load_acc2.wait()
        gs[layers] = d_out[0]
        backward(True, False)
        dxs[1] = gs[0]
        send_dx1.start()
        forward(0, False)
        send_cot.wait_recv()
        gs[layers] = cot_in[...]
        backward(False, True, send_dx0)
        dxs[0] = gs[0]
        send_dx1.wait_send()
        send_dx0.wait_send()

    dx_out[...] = dxs[...]

    def drain(i, carry):
        red1.drain(i)
        red2.drain(i)
        return carry

    lax.fori_loop(0, layers, drain, 0)


def mlp(d_out, stored_x, w_in, w_out, acc_in, acc_out):
    layers, hid, ff = w_in.shape
    tokens = d_out.shape[1]
    n1, n2 = hid // 8, ff // 8
    return pl.pallas_call(
        functools.partial(mlp_kernel, layers, 1),
        out_shape=(jax.ShapeDtypeStruct((layers, n1, ff), F32), jax.ShapeDtypeStruct((layers, n2, hid), F32),
                   jax.ShapeDtypeStruct((2, tokens, hid), BF16)),
        in_specs=[VM, VM, ANY, ANY, ANY, ANY],
        out_specs=(VM, VM, VM),
        scratch_shapes=[
            pltpu.VMEM((layers, hid, ff), BF16),
            pltpu.VMEM((layers, ff, hid), BF16),
            pltpu.VMEM((layers + 1, tokens, hid), BF16),
            pltpu.VMEM((layers, tokens, ff), BF16),
            pltpu.VMEM((layers, tokens, ff), F32),
            pltpu.VMEM((layers + 1, tokens, hid), BF16),
            pltpu.VMEM((tokens, ff), BF16),
            pltpu.VMEM((layers, hid, ff), F32),
            pltpu.VMEM((layers, hid, ff), F32),
            pltpu.VMEM((layers, ff, hid), F32),
            pltpu.VMEM((tokens, hid), BF16),
            pltpu.VMEM((2, tokens, hid), BF16),
            pltpu.VMEM((layers, 8, n1, ff), BF16),
            pltpu.VMEM((layers, 4, n1, ff), BF16),
            pltpu.VMEM((layers, 2, n1, ff), BF16),
            pltpu.VMEM((layers, n1, ff), BF16),
            pltpu.VMEM((layers, 8, n2, hid), BF16),
            pltpu.VMEM((layers, 4, n2, hid), BF16),
            pltpu.VMEM((layers, 2, n2, hid), BF16),
            pltpu.VMEM((layers, n2, hid), BF16),
            pltpu.SemaphoreType.DMA((2, layers)),
            pltpu.SemaphoreType.DMA((2,)),
            pltpu.SemaphoreType.DMA((6,)),
            pltpu.SemaphoreType.DMA((6, layers)),
            pltpu.SemaphoreType.DMA((6, layers)),
        ],
        compiler_params=pltpu.CompilerParams(collective_id=0, has_side_effects=True, vmem_limit_bytes=63 * 2**20),
    )(d_out, stored_x, w_in, w_out, acc_in, acc_out)


def emb_kernel(pairs, width, rel_ids, dx, acc, out, buf, dxt, sa, sa0, sa1, sa2, sb, sb0, sb1, sb2, fa, fb, za, zb,
               asem, sema, semb, zsem):
    pp, y, x, c, to_x, to_y, to_c, to_z = coords()
    half = 2 * pairs * width
    vocab = acc.shape[0]
    block = 256

    def load(p, size, base):
        return pltpu.make_async_copy(acc.at[pl.ds(base + p * 2 * width, size), 0, :], buf.at[pl.ds(p * 2 * width, size)], asem.at[p])

    def each_load(act):
        for p in range(pairs):
            tail = vocab - half - p * 2 * width
            @pl.when(pp == 0)
            def _():
                act(load(p, 2 * width, 0))

            if tail > 0:
                @pl.when(pp == 1)
                def _():
                    act(load(p, min(2 * width, tail), half))

    each_load(lambda cp: cp.start())
    enter((to_x, to_y, to_c, to_z))
    dxt[...] = dx[...].T
    each_load(lambda cp: cp.wait())

    reda = Reduce(sa, sa0, sa1, sa2, sema, (to_c, to_x, to_y), c, x, y)
    redb = Reduce(sb, sb0, sb1, sb2, semb, (to_c, to_y, to_x), c, y, x)

    def zcopy(i):
        return (remote(fa.at[i], za.at[i], zsem.at[0, i], zsem.at[1, i], to_z),
                remote(fb.at[i], zb.at[i], zsem.at[2, i], zsem.at[3, i], to_z))

    def build(i):
        for part, dst, slab in ((0, sa, slab_xy), (1, sb, slab_yx)):
            def piece(j, carry):
                at = pl.multiple_of(j * block, block)
                row = pl.multiple_of((2 * i + part) * width + j * block, block)
                base = pp * half + row
                ids = rel_ids[...]
                hot = jnp.concatenate([jnp.where(ids == base + 128 * n, 1.0, 0.0).astype(BF16) for n in range(block // 128)], axis=1)
                val = buf[pl.ds(row, block), :].T + dot(dxt[...], hot, 1, 0)
                val = val.astype(BF16)
                for d in range(8):
                    dst[i, slab(d), :, pl.ds(at, block)] = val[d * 16:(d + 1) * 16]
                return carry

            lax.fori_loop(0, width // block, piece, 0)

    def stage(k, lag, fn):
        @pl.when((k >= lag) & (k < pairs + lag))
        def _():
            fn(k - lag)

    def step(k, carry):
        stage(k, 1, lambda i: (reda.copy0(i).start(), redb.copy0(i).start()))
        stage(k, 2, lambda i: (reda.copy1(i).start(), redb.copy1(i).start()))
        stage(k, 4, lambda i: (reda.copy2(i).start(), redb.copy2(i).start()))
        stage(k, 6, lambda i: [cp.start() for cp in zcopy(i)])
        stage(k, 0, build)
        stage(k, 1, lambda i: (reda.add0(i), redb.add0(i)))
        stage(k, 3, lambda i: (reda.add1(i), redb.add1(i)))

        def finish(i):
            fa[i] = reda.last(i).astype(BF16)
            fb[i] = redb.last(i).astype(BF16)

        stage(k, 5, finish)
        return carry

    lax.fori_loop(0, pairs + 7, step, 0)

    def put(i, carry):
        for cp in zcopy(i):
            cp.wait_recv()
        for part, mine, other in ((0, fa, za), (1, fb, zb)):
            off = (2 * i + part) * width
            out[:, pl.ds(pl.multiple_of(pp * half + off, 128), width)] = mine[i]
            out[:, pl.ds(pl.multiple_of((1 - pp) * half + off, 128), width)] = other[i]
        reda.drain(i)
        redb.drain(i)
        for cp in zcopy(i):
            cp.wait_send()
        return carry

    lax.fori_loop(0, pairs, put, 0)


def embed(rel_ids, dx, acc_emb):
    vocab, _, hid = acc_emb.shape
    pairs, width = 6, 1280
    half = 2 * pairs * width
    n = hid // 8
    side = [
        pltpu.VMEM((pairs, 8, n, width), BF16),
        pltpu.VMEM((pairs, 4, n, width), BF16),
        pltpu.VMEM((pairs, 2, n, width), BF16),
        pltpu.VMEM((pairs, n, width), BF16),
    ]
    piece = pltpu.VMEM((pairs, n, width), BF16)
    return pl.pallas_call(
        functools.partial(emb_kernel, pairs, width),
        out_shape=jax.ShapeDtypeStruct((n, 2 * half), BF16),
        in_specs=[VM, VM, ANY],
        out_specs=VM,
        scratch_shapes=[
            pltpu.VMEM((half, hid), F32),
            pltpu.VMEM((hid, dx.shape[0]), BF16),
            *side, *side, piece, piece, piece, piece,
            pltpu.SemaphoreType.DMA((pairs,)),
            pltpu.SemaphoreType.DMA((6, pairs)),
            pltpu.SemaphoreType.DMA((6, pairs)),
            pltpu.SemaphoreType.DMA((4, pairs)),
        ],
        compiler_params=pltpu.CompilerParams(collective_id=1, has_side_effects=True, vmem_limit_bytes=63 * 2**20),
    )(rel_ids, dx, acc_emb)


def solution(mesh):
    def device_body(tok_ids, d_out, stored_x, w_in, w_out, acc_in, acc_out, acc_emb):
        grad_in, grad_out, dx = mlp(d_out, stored_x, w_in, w_out, acc_in, acc_out)
        vocab, hid = acc_emb.shape[1:]
        lane = lax.broadcasted_iota(jnp.int32, (1, 128), 1)
        rel_ids = tok_ids.reshape(-1, 1) - lane
        total = embed(rel_ids, dx.reshape(-1, hid), acc_emb.reshape(vocab, 1, hid))
        grad_emb = total[:, :vocab].T.astype(F32) * 0.125
        return grad_in, grad_out, grad_emb

    return jax.shard_map(
        device_body,
        mesh=mesh,
        in_specs=(P(None, "dp"), P("pp", "dp", None), P("pp", None, "dp", None), P("pp", None, None), P("pp", None, None),
                  P("pp", "dp", None, None), P("pp", "dp", None, None), P("dp", None, None)),
        out_specs=(P("pp", "dp", None), P("pp", "dp", None), P(None, "dp")),
        check_vma=False,
    )
```

```python
import functools

import jax
import jax.numpy as jnp
from jax import lax
from jax.experimental import pallas as pl
from jax.experimental.pallas import tpu as pltpu
from jax.sharding import PartitionSpec as P

MESH = pl.DeviceIdType.MESH
C0 = 0.7978845608028654
C1 = 0.044715
F32, BF16 = jnp.float32, jnp.bfloat16
ANY = pl.BlockSpec(memory_space=pl.ANY)
VM = pl.BlockSpec(memory_space=pltpu.VMEM)


def coords():
    pp, d = lax.axis_index("pp"), lax.axis_index("dp")
    y, x, c = d // 4, (d // 2) % 2, d % 2
    to_x = {"pp": pp, "dp": d + 2 - 4 * x}
    to_y = {"pp": pp, "dp": d + 4 - 8 * y}
    to_c = {"pp": pp, "dp": d + 1 - 2 * c}
    to_z = {"pp": 1 - pp, "dp": d}
    return pp, y, x, c, to_x, to_y, to_c, to_z


def enter(neighbours):
    barrier = pltpu.get_barrier_semaphore()
    for dev in neighbours:
        pl.semaphore_signal(barrier, inc=1, device_id=dev, device_id_type=MESH)
    pl.semaphore_wait(barrier, len(neighbours))


def remote(src, dst, send, recv, dev):
    return pltpu.make_async_remote_copy(src_ref=src, dst_ref=dst, send_sem=send, recv_sem=recv, device_id=dev, device_id_type=MESH)


def slab_xy(d):
    return (d % 2) * 4 + ((d // 2) % 2) * 2 + d // 4


def slab_yx(d):
    return (d % 2) * 4 + (d // 4) * 2 + (d // 2) % 2


class Reduce:
    def __init__(self, src, r0, r1, r2, sems, to, c, p, q):
        self.src, self.r0, self.r1, self.r2, self.sems, self.to = src, r0, r1, r2, sems, to
        self.c, self.p, self.q = c, p, q

    def copy0(self, i):
        return remote(self.src.at[i, pl.ds(4 * (1 - self.c), 4)], self.r0.at[i], self.sems.at[0, i], self.sems.at[1, i], self.to[0])

    def copy1(self, i):
        at = 4 * self.c + 2 * (1 - self.p)
        return remote(self.src.at[i, pl.ds(at, 2)], self.r1.at[i], self.sems.at[2, i], self.sems.at[3, i], self.to[1])

    def copy2(self, i):
        at = 4 * self.c + 2 * self.p + 1 - self.q
        return remote(self.src.at[i, at], self.r2.at[i], self.sems.at[4, i], self.sems.at[5, i], self.to[2])

    def add0(self, i):
        self.copy0(i).wait_recv()
        for k in range(4):
            at = 4 * self.c + k
            self.src[i, at] = (self.src[i, at].astype(F32) + self.r0[i, k].astype(F32)).astype(BF16)

    def add1(self, i):
        self.copy1(i).wait_recv()
        for k in range(2):
            at = 4 * self.c + 2 * self.p + k
            self.src[i, at] = (self.src[i, at].astype(F32) + self.r1[i, k].astype(F32)).astype(BF16)

    def last(self, i):
        self.copy2(i).wait_recv()
        at = 4 * self.c + 2 * self.p + self.q
        return self.src[i, at].astype(F32) + self.r2[i].astype(F32)

    def drain(self, i):
        self.copy0(i).wait_send()
        self.copy1(i).wait_send()
        self.copy2(i).wait_send()


def dot(a, b, ca, cb):
    return lax.dot_general(a, b, (((ca,), (cb,)), ((), ())), preferred_element_type=F32)


def fused_kernel(layers, pairs, width, vocab, tok_ids, d_out, x_in, w_in, w_out, acc_in, acc_out, acc_emb, g_in, g_out, emb_out,
                 w1, w2, xs, hid, slope, gs, dh, dw1, dw2, acc2, cot_in, dxs, s1, s1a, s1b, s1c, s2, s2a, s2b, s2c,
                 rel, buf, dxt, sa, sa0, sa1, sa2, sb, sb0, sb1, sb2, fa, fb, za, zb,
                 wsem, asem, zsem, sem1, sem2, esem, sema, semb, fsem):
    pp, y, x, c, to_x, to_y, to_c, to_z = coords()
    tokens = dxs.shape[1]
    half = 2 * pairs * width
    block = 256

    def load(i):
        return (pltpu.make_async_copy(w_in.at[i], w1.at[i], wsem.at[0, i]),
                pltpu.make_async_copy(w_out.at[i], w2.at[i], wsem.at[1, i]))

    def load_emb(act):
        def one(size, base):
            act(pltpu.make_async_copy(acc_emb.at[pl.ds(base, size), 0, :], buf.at[pl.ds(0, size)], esem))

        @pl.when(pp == 0)
        def _():
            one(half, 0)

        @pl.when(pp == 1)
        def _():
            one(vocab - half, half)

    load_x = pltpu.make_async_copy(x_in.at[0, 1 - pp], xs.at[0], asem.at[2])
    load_g = pltpu.make_async_copy(d_out.at[0], gs.at[layers], asem.at[3])
    load_x.start()
    load_g.start()
    load_acc1 = pltpu.make_async_copy(acc_in.at[:, 0], dw1, asem.at[0])
    load_acc2 = pltpu.make_async_copy(acc_out.at[:, 0], acc2, asem.at[1])
    for i in range(layers):
        for cp in load(i):
            cp.start()
    load_acc1.start()
    load_acc2.start()
    load_emb(lambda cp: cp.start())
    enter((to_x, to_y, to_c, to_z))

    lane = lax.broadcasted_iota(jnp.int32, (128, 128), 1)
    for j in range(2):
        for b in range(tokens // 128):
            ids = tok_ids[j:j + 1, b * 128:(b + 1) * 128].astype(F32)
            ids = jnp.broadcast_to(ids, (128, 128)).T.astype(jnp.int32)
            rel[pl.ds(j * tokens + b * 128, 128)] = ids - lane
    load_x.wait()

    red1 = Reduce(s1, s1a, s1b, s1c, sem1, (to_c, to_x, to_y), c, x, y)
    red2 = Reduce(s2, s2a, s2b, s2c, sem2, (to_c, to_y, to_x), c, y, x)
    reda = Reduce(sa, sa0, sa1, sa2, sema, (to_c, to_x, to_y), c, x, y)
    redb = Reduce(sb, sb0, sb1, sb2, semb, (to_c, to_y, to_x), c, y, x)

    def forward(fresh):
        def body(i, carry):
            if fresh:
                for cp in load(i):
                    cp.wait()
            xc = xs[i]
            h = dot(xc, w1[i], 1, 0).astype(BF16).astype(F32)
            h2 = h * h
            t = jnp.tanh(h * (C0 + (C0 * C1) * h2))
            cdf = 0.5 + 0.5 * t
            a = (h * cdf).astype(BF16)
            hid[i] = a
            slope[i] = cdf + h * ((cdf * (1.0 - cdf)) * (2.0 * C0 + (6.0 * C0 * C1) * h2))
            xs[i + 1] = (xc.astype(F32) + dot(a, w2[i], 1, 0)).astype(BF16)
            return carry

        lax.fori_loop(0, layers, body, 0)

    def block_backward(i, first, final):
        gc = gs[i + 1]
        da = dot(gc, w2[i], 1, 1).astype(BF16).astype(F32)
        dhc = (da * slope[i]).astype(BF16)
        dh[...] = dhc
        gs[i] = (gc.astype(F32) + dot(dhc, w1[i], 1, 1)).astype(BF16)
        new2 = dot(gs[i + 1], hid[i], 0, 0)
        if not first:
            new2 = new2 + dw2[i]
        new1 = dot(xs[i], dh[...], 0, 0) + dw1[i]
        if not final:
            dw1[i] = new1
            dw2[i] = new2
            return
        new1 = new1.astype(BF16)
        n1 = new1.shape[0] // 8
        for d in range(8):
            s1[i, slab_xy(d)] = new1[d * n1:(d + 1) * n1]
        new2 = (new2.T + acc2[i]).astype(BF16)
        n2 = new2.shape[0] // 8
        for d in range(8):
            s2[i, slab_yx(d)] = new2[d * n2:(d + 1) * n2]

    def start0(i):
        red1.copy0(i).start()
        red2.copy0(i).start()

    def start1(i):
        red1.copy1(i).start()
        red2.copy1(i).start()

    def start2(i):
        red1.copy2(i).start()
        red2.copy2(i).start()

    def add0(i):
        red1.add0(i)
        red2.add0(i)

    def add1(i):
        red1.add1(i)
        red2.add1(i)

    def finish(i):
        g_in[i] = red1.last(i)
        g_out[i] = red2.last(i)

    def when_layer(k, lag, fn):
        @pl.when((k >= lag) & (k < layers + lag))
        def _():
            fn(layers - 1 - (k - lag))

    send_cot = remote(gs.at[0], cot_in, zsem.at[0], zsem.at[1], to_z)
    send_dx1 = remote(dxs.at[1], dxs.at[1], zsem.at[2], zsem.at[3], to_z)
    send_dx0 = remote(gs.at[0], dxs.at[0], zsem.at[4], zsem.at[5], to_z)

    @pl.when(pp == 1)
    def _():
        forward(True)
        load_acc1.wait()
        load_acc2.wait()
        load_g.wait()

        def step(k, carry):
            @pl.when(k == layers)
            def _():
                send_cot.start()

            when_layer(k, 1, start0)
            when_layer(k, 3, start1)
            when_layer(k, 6, start2)
            when_layer(k, 0, lambda i: block_backward(i, True, True))
            when_layer(k, 2, add0)
            when_layer(k, 5, add1)
            when_layer(k, 8, finish)
            return carry

        lax.fori_loop(0, layers + 9, step, 0)
        send_cot.wait_send()
        send_dx1.wait_recv()
        dxt[:, pl.ds(tokens, tokens)] = dxs[1].T
        send_dx0.wait_recv()
        dxt[:, pl.ds(0, tokens)] = dxs[0].T

    @pl.when(pp == 0)
    def _():
        next_x = pltpu.make_async_copy(x_in.at[0, 0], dxs.at[0], asem.at[4])
        next_x.start()
        forward(True)
        load_acc1.wait()
        load_acc2.wait()
        load_g.wait()

        def back(k, carry):
            block_backward(layers - 1 - k, True, False)
            return carry

        lax.fori_loop(0, layers, back, 0)
        dxs[1] = gs[0]
        send_dx1.start()
        next_x.wait()
        xs[0] = dxs[0]
        forward(False)
        dxt[:, pl.ds(tokens, tokens)] = dxs[1].T
        send_cot.wait_recv()
        gs[layers] = cot_in[...]

        def step(k, carry):
            @pl.when(k == layers)
            def _():
                send_dx0.start()

            when_layer(k, 1, start0)
            when_layer(k, 3, start1)
            when_layer(k, 0, lambda i: block_backward(i, False, True))
            when_layer(k, 2, add0)
            return carry

        lax.fori_loop(0, layers + 4, step, 0)
        dxt[:, pl.ds(0, tokens)] = gs[0].T
        send_dx1.wait_send()
        send_dx0.wait_send()

    load_emb(lambda cp: cp.wait())

    def zcopy(i):
        return (remote(fa.at[i], za.at[i], fsem.at[0, i], fsem.at[1, i], to_z),
                remote(fb.at[i], zb.at[i], fsem.at[2, i], fsem.at[3, i], to_z))

    def build(i):
        for part, dst, slab in ((0, sa, slab_xy), (1, sb, slab_yx)):
            def piece(j, carry):
                at = pl.multiple_of(j * block, block)
                row = pl.multiple_of((2 * i + part) * width + j * block, block)
                base = pp * half + row
                ids = rel[...]
                hot = jnp.concatenate([jnp.where(ids == base + 128 * n, 1.0, 0.0).astype(BF16) for n in range(block // 128)], axis=1)
                val = buf[pl.ds(row, block), :].T + dot(dxt[...], hot, 1, 0)
                val = val.astype(BF16)
                for d in range(8):
                    dst[i, slab(d), :, pl.ds(at, block)] = val[d * 16:(d + 1) * 16]
                return carry

            lax.fori_loop(0, width // block, piece, 0)

    def emb_finish(i):
        fa[i] = reda.last(i).astype(BF16)
        fb[i] = redb.last(i).astype(BF16)

    def put(i):
        for cp in zcopy(i):
            cp.wait_recv()
        for part, mine, other in ((0, fa, za), (1, fb, zb)):
            off = (2 * i + part) * width
            emb_out[:, pl.ds(pl.multiple_of(pp * half + off, 128), width)] = mine[i]
            emb_out[:, pl.ds(pl.multiple_of((1 - pp) * half + off, 128), width)] = other[i]

    def emb_step(k, carry):
        def stage(lag, fn):
            @pl.when((k >= lag) & (k < pairs + lag))
            def _():
                fn(k - lag)

        def late(lag, fn):
            for n in range(2):
                at = 2 * (k - lag) + n

                @pl.when((pp == 0) & (at >= 0) & (at < layers))
                def _():
                    fn(layers - 1 - at)

        late(1, start2)
        stage(1, lambda i: (reda.copy0(i).start(), redb.copy0(i).start()))
        stage(2, lambda i: (reda.copy1(i).start(), redb.copy1(i).start()))
        stage(4, lambda i: (reda.copy2(i).start(), redb.copy2(i).start()))
        stage(6, lambda i: [cp.start() for cp in zcopy(i)])
        stage(0, build)
        late(0, add1)
        stage(1, lambda i: (reda.add0(i), redb.add0(i)))
        stage(3, lambda i: (reda.add1(i), redb.add1(i)))
        stage(5, emb_finish)
        late(4, finish)
        stage(8, put)
        return carry

    lax.fori_loop(0, pairs + 9, emb_step, 0)

    def drain_layer(i, carry):
        red1.drain(i)
        red2.drain(i)
        return carry

    lax.fori_loop(0, layers, drain_layer, 0)

    def drain_pair(i, carry):
        reda.drain(i)
        redb.drain(i)
        for cp in zcopy(i):
            cp.wait_send()
        return carry

    lax.fori_loop(0, pairs, drain_pair, 0)


def fused(tok_ids, d_out, stored_x, w_in, w_out, acc_in, acc_out, acc_emb):
    layers, hid, ff = w_in.shape
    tokens = d_out.shape[1]
    vocab = acc_emb.shape[0]
    pairs, width = 10, 768
    half = 2 * pairs * width
    n1, n2 = hid // 8, ff // 8

    def side(count, *shape):
        return [pltpu.VMEM((count, 8, *shape), BF16), pltpu.VMEM((count, 4, *shape), BF16),
                pltpu.VMEM((count, 2, *shape), BF16), pltpu.VMEM((count, *shape), BF16)]

    piece = pltpu.VMEM((pairs, n1, width), BF16)
    return pl.pallas_call(
        functools.partial(fused_kernel, layers, pairs, width, vocab),
        out_shape=(jax.ShapeDtypeStruct((layers, n1, ff), F32), jax.ShapeDtypeStruct((layers, n2, hid), F32),
                   jax.ShapeDtypeStruct((n1, 2 * half), BF16)),
        in_specs=[VM, ANY, ANY, ANY, ANY, ANY, ANY, ANY],
        out_specs=(VM, VM, VM),
        scratch_shapes=[
            pltpu.VMEM((layers, hid, ff), BF16),
            pltpu.VMEM((layers, ff, hid), BF16),
            pltpu.VMEM((layers + 1, tokens, hid), BF16),
            pltpu.VMEM((layers, tokens, ff), BF16),
            pltpu.VMEM((layers, tokens, ff), F32),
            pltpu.VMEM((layers + 1, tokens, hid), BF16),
            pltpu.VMEM((tokens, ff), BF16),
            pltpu.VMEM((layers, hid, ff), F32),
            pltpu.VMEM((layers, hid, ff), F32),
            pltpu.VMEM((layers, ff, hid), F32),
            pltpu.VMEM((tokens, hid), BF16),
            pltpu.VMEM((2, tokens, hid), BF16),
            *side(layers, n1, ff),
            *side(layers, n2, hid),
            pltpu.VMEM((2 * tokens, 128), jnp.int32),
            pltpu.VMEM((half, hid), F32),
            pltpu.VMEM((hid, 2 * tokens), BF16),
            *side(pairs, n1, width),
            *side(pairs, n1, width),
            piece, piece, piece, piece,
            pltpu.SemaphoreType.DMA((2, layers)),
            pltpu.SemaphoreType.DMA((5,)),
            pltpu.SemaphoreType.DMA((6,)),
            pltpu.SemaphoreType.DMA((6, layers)),
            pltpu.SemaphoreType.DMA((6, layers)),
            pltpu.SemaphoreType.DMA,
            pltpu.SemaphoreType.DMA((6, pairs)),
            pltpu.SemaphoreType.DMA((6, pairs)),
            pltpu.SemaphoreType.DMA((4, pairs)),
        ],
        compiler_params=pltpu.CompilerParams(collective_id=0, has_side_effects=True, vmem_limit_bytes=67043328),
    )(tok_ids, d_out, stored_x, w_in, w_out, acc_in, acc_out, acc_emb)


def mean_kernel(a, b, e, g_in, g_out, g_emb):
    g_in[...] = a[...] * 0.125
    g_out[...] = b[...] * 0.125
    g_emb[...] = e[:, :g_emb.shape[1]].astype(F32) * 0.125


def mean(a, b, e, vocab):
    return pl.pallas_call(
        mean_kernel,
        out_shape=(jax.ShapeDtypeStruct(a.shape, F32), jax.ShapeDtypeStruct(b.shape, F32), jax.ShapeDtypeStruct((e.shape[0], vocab), F32)),
        in_specs=[VM, VM, VM],
        out_specs=(VM, VM, VM),
    )(a, b, e)


def solution(mesh):
    def device_body(tok_ids, d_out, stored_x, w_in, w_out, acc_in, acc_out, acc_emb):
        vocab, hid = acc_emb.shape[1:]
        sums = fused(tok_ids, d_out, stored_x, w_in, w_out, acc_in, acc_out, acc_emb.reshape(vocab, 1, hid))
        grad_in, grad_out, grad_emb = mean(*sums, vocab)
        return grad_in, grad_out, grad_emb.T

    return jax.shard_map(
        device_body,
        mesh=mesh,
        in_specs=(P(None, "dp"), P("pp", "dp", None), P("pp", None, "dp", None), P("pp", None, None), P("pp", None, None),
                  P("pp", "dp", None, None), P("pp", "dp", None, None), P("dp", None, None)),
        out_specs=(P("pp", "dp", None), P("pp", "dp", None), P(None, "dp")),
        check_vma=False,
    )
```

```python
import functools

import jax
import jax.numpy as jnp
from jax import lax
from jax.experimental import pallas as pl
from jax.experimental.pallas import tpu as pltpu
from jax.sharding import PartitionSpec as P

MESH = pl.DeviceIdType.MESH
C0 = 0.7978845608028654
C1 = 0.044715
F32, BF16 = jnp.float32, jnp.bfloat16
ANY = pl.BlockSpec(memory_space=pl.ANY)
VM = pl.BlockSpec(memory_space=pltpu.VMEM)


def coords():
    pp, d = lax.axis_index("pp"), lax.axis_index("dp")
    y, x, c = d // 4, (d // 2) % 2, d % 2
    to_x = {"pp": pp, "dp": d + 2 - 4 * x}
    to_y = {"pp": pp, "dp": d + 4 - 8 * y}
    to_c = {"pp": pp, "dp": d + 1 - 2 * c}
    to_z = {"pp": 1 - pp, "dp": d}
    return pp, y, x, c, to_x, to_y, to_c, to_z


def enter(neighbours):
    barrier = pltpu.get_barrier_semaphore()
    for dev in neighbours:
        pl.semaphore_signal(barrier, inc=1, device_id=dev, device_id_type=MESH)
    pl.semaphore_wait(barrier, len(neighbours))


def remote(src, dst, send, recv, dev):
    return pltpu.make_async_remote_copy(src_ref=src, dst_ref=dst, send_sem=send, recv_sem=recv, device_id=dev, device_id_type=MESH)


def slab_xy(d):
    return (d % 2) * 4 + ((d // 2) % 2) * 2 + d // 4


def slab_yx(d):
    return (d % 2) * 4 + (d // 4) * 2 + (d // 2) % 2


class Reduce:
    def __init__(self, src, r0, r1, r2, sems, to, c, p, q):
        self.src, self.r0, self.r1, self.r2, self.sems, self.to = src, r0, r1, r2, sems, to
        self.c, self.p, self.q = c, p, q

    def copy0(self, i):
        return remote(self.src.at[i, pl.ds(4 * (1 - self.c), 4)], self.r0.at[i], self.sems.at[0, i], self.sems.at[1, i], self.to[0])

    def copy1(self, i):
        at = 4 * self.c + 2 * (1 - self.p)
        return remote(self.src.at[i, pl.ds(at, 2)], self.r1.at[i], self.sems.at[2, i], self.sems.at[3, i], self.to[1])

    def copy2(self, i):
        at = 4 * self.c + 2 * self.p + 1 - self.q
        return remote(self.src.at[i, at], self.r2.at[i], self.sems.at[4, i], self.sems.at[5, i], self.to[2])

    def add0(self, i):
        self.copy0(i).wait_recv()
        for k in range(4):
            at = 4 * self.c + k
            self.src[i, at] = (self.src[i, at].astype(F32) + self.r0[i, k].astype(F32)).astype(BF16)

    def add1(self, i):
        self.copy1(i).wait_recv()
        for k in range(2):
            at = 4 * self.c + 2 * self.p + k
            self.src[i, at] = (self.src[i, at].astype(F32) + self.r1[i, k].astype(F32)).astype(BF16)

    def last(self, i):
        self.copy2(i).wait_recv()
        at = 4 * self.c + 2 * self.p + self.q
        return self.src[i, at].astype(F32) + self.r2[i].astype(F32)

    def drain(self, i):
        self.copy0(i).wait_send()
        self.copy1(i).wait_send()
        self.copy2(i).wait_send()


def dot(a, b, ca, cb):
    return lax.dot_general(a, b, (((ca,), (cb,)), ((), ())), preferred_element_type=F32)


def fused_kernel(layers, pairs, width, vocab, tok_ids, d_out, x_in, w_in, w_out, acc_in, acc_out, acc_emb, g_in, g_out, emb_out,
                 w1, w2, xs, hid, slope, gs, dh, dw1, dw2, acc2, cot_in, dxs, s1, s1a, s1b, s1c, s2, s2a, s2b, s2c,
                 rel, buf, dxt, sa, sa0, sa1, sa2, sb, sb0, sb1, sb2, fa, fb, za, zb,
                 wsem, asem, zsem, sem1, sem2, esem, sema, semb, fsem):
    pp, y, x, c, to_x, to_y, to_c, to_z = coords()
    tokens = dxs.shape[1]
    half = 2 * pairs * width
    block = width

    def load(i):
        return (pltpu.make_async_copy(w_in.at[i], w1.at[i], wsem.at[0, i]),
                pltpu.make_async_copy(w_out.at[i], w2.at[i], wsem.at[1, i]))

    def load_emb(act):
        def one(size, base):
            act(pltpu.make_async_copy(acc_emb.at[pl.ds(base, size), 0, :], buf.at[pl.ds(0, size)], esem))

        @pl.when(pp == 0)
        def _():
            one(half, 0)

        @pl.when(pp == 1)
        def _():
            one(vocab - half, half)

    load_x = pltpu.make_async_copy(x_in.at[0, 1 - pp], xs.at[0], asem.at[2])
    load_g = pltpu.make_async_copy(d_out.at[0], gs.at[layers], asem.at[3])
    load_x.start()
    load_g.start()
    load_acc1 = pltpu.make_async_copy(acc_in.at[:, 0], dw1, asem.at[0])
    load_acc2 = pltpu.make_async_copy(acc_out.at[:, 0], acc2, asem.at[1])
    for i in range(layers):
        for cp in load(i):
            cp.start()
    load_acc1.start()
    load_acc2.start()
    load_emb(lambda cp: cp.start())
    enter((to_x, to_y, to_c, to_z))

    lane = lax.broadcasted_iota(jnp.int32, (128, 128), 1)
    for j in range(2):
        for b in range(tokens // 128):
            ids = tok_ids[j:j + 1, b * 128:(b + 1) * 128].astype(F32)
            ids = jnp.broadcast_to(ids, (128, 128)).T.astype(jnp.int32)
            rel[pl.ds(j * tokens + b * 128, 128)] = ids - lane
    load_x.wait()

    red1 = Reduce(s1, s1a, s1b, s1c, sem1, (to_c, to_x, to_y), c, x, y)
    red2 = Reduce(s2, s2a, s2b, s2c, sem2, (to_c, to_y, to_x), c, y, x)
    reda = Reduce(sa, sa0, sa1, sa2, sema, (to_c, to_x, to_y), c, x, y)
    redb = Reduce(sb, sb0, sb1, sb2, semb, (to_c, to_y, to_x), c, y, x)

    def forward(fresh):
        def body(i, carry):
            if fresh:
                for cp in load(i):
                    cp.wait()
            xc = xs[i]
            h = dot(xc, w1[i], 1, 0).astype(BF16).astype(F32)
            h2 = h * h
            t = jnp.tanh(h * (C0 + (C0 * C1) * h2))
            cdf = 0.5 + 0.5 * t
            a = (h * cdf).astype(BF16)
            hid[i] = a
            slope[i] = cdf + h * ((cdf * (1.0 - cdf)) * (2.0 * C0 + (6.0 * C0 * C1) * h2))
            xs[i + 1] = (xc.astype(F32) + dot(a, w2[i], 1, 0)).astype(BF16)
            return carry

        lax.fori_loop(0, layers, body, 0)

    def block_backward(i, first, final):
        gc = gs[i + 1]
        da = dot(gc, w2[i], 1, 1).astype(BF16).astype(F32)
        dhc = (da * slope[i]).astype(BF16)
        dh[...] = dhc
        gs[i] = (gc.astype(F32) + dot(dhc, w1[i], 1, 1)).astype(BF16)
        new2 = dot(gs[i + 1], hid[i], 0, 0)
        if not first:
            new2 = new2 + dw2[i]
        new1 = dot(xs[i], dh[...], 0, 0) + dw1[i]
        if not final:
            dw1[i] = new1
            dw2[i] = new2
            return
        new1 = new1.astype(BF16)
        n1 = new1.shape[0] // 8
        for d in range(8):
            s1[i, slab_xy(d)] = new1[d * n1:(d + 1) * n1]
        new2 = (new2.T + acc2[i]).astype(BF16)
        n2 = new2.shape[0] // 8
        for d in range(8):
            s2[i, slab_yx(d)] = new2[d * n2:(d + 1) * n2]

    def start0(i):
        red1.copy0(i).start()
        red2.copy0(i).start()

    def start1(i):
        red1.copy1(i).start()
        red2.copy1(i).start()

    def start2(i):
        red1.copy2(i).start()
        red2.copy2(i).start()

    def add0(i):
        red1.add0(i)
        red2.add0(i)

    def add1(i):
        red1.add1(i)
        red2.add1(i)

    def finish(i):
        g_in[i] = red1.last(i)
        g_out[i] = red2.last(i)

    def when_layer(k, lag, fn):
        @pl.when((k >= lag) & (k < layers + lag))
        def _():
            fn(layers - 1 - (k - lag))

    send_cot = remote(gs.at[0], cot_in, zsem.at[0], zsem.at[1], to_z)
    send_dx1 = remote(dxs.at[1], dxs.at[1], zsem.at[2], zsem.at[3], to_z)
    send_dx0 = remote(gs.at[0], dxs.at[0], zsem.at[4], zsem.at[5], to_z)

    @pl.when(pp == 1)
    def _():
        forward(True)
        load_acc1.wait()
        load_acc2.wait()
        load_g.wait()

        def step(k, carry):
            @pl.when(k == layers)
            def _():
                send_cot.start()

            when_layer(k, 1, start0)
            when_layer(k, 3, start1)
            when_layer(k, 6, start2)
            when_layer(k, 0, lambda i: block_backward(i, True, True))
            when_layer(k, 2, add0)
            when_layer(k, 5, add1)
            when_layer(k, 8, finish)
            return carry

        lax.fori_loop(0, layers + 9, step, 0)
        send_cot.wait_send()
        send_dx1.wait_recv()
        dxt[:, pl.ds(tokens, tokens)] = dxs[1].T
        send_dx0.wait_recv()
        dxt[:, pl.ds(0, tokens)] = dxs[0].T

    @pl.when(pp == 0)
    def _():
        next_x = pltpu.make_async_copy(x_in.at[0, 0], dxs.at[0], asem.at[4])
        next_x.start()
        forward(True)
        load_acc1.wait()
        load_acc2.wait()
        load_g.wait()

        def back(k, carry):
            block_backward(layers - 1 - k, True, False)
            return carry

        lax.fori_loop(0, layers, back, 0)
        dxs[1] = gs[0]
        send_dx1.start()
        next_x.wait()
        xs[0] = dxs[0]
        forward(False)
        dxt[:, pl.ds(tokens, tokens)] = dxs[1].T
        send_cot.wait_recv()
        gs[layers] = cot_in[...]

        def step(k, carry):
            @pl.when(k == layers)
            def _():
                send_dx0.start()

            when_layer(k, 1, start0)
            when_layer(k, 3, start1)
            when_layer(k, 0, lambda i: block_backward(i, False, True))
            when_layer(k, 2, add0)
            return carry

        lax.fori_loop(0, layers + 4, step, 0)
        dxt[:, pl.ds(0, tokens)] = gs[0].T
        send_dx1.wait_send()
        send_dx0.wait_send()

    load_emb(lambda cp: cp.wait())

    def zcopy(i):
        return (remote(fa.at[i], za.at[i], fsem.at[0, i], fsem.at[1, i], to_z),
                remote(fb.at[i], zb.at[i], fsem.at[2, i], fsem.at[3, i], to_z))

    def build(i):
        for part, dst, slab in ((0, sa, slab_xy), (1, sb, slab_yx)):
            def piece(j, carry):
                at = pl.multiple_of(j * block, block)
                row = pl.multiple_of((2 * i + part) * width + j * block, block)
                base = pp * half + row
                ids = rel[...]
                hot = jnp.concatenate([jnp.where(ids == base + 128 * n, 1.0, 0.0).astype(BF16) for n in range(block // 128)], axis=1)
                val = buf[pl.ds(row, block), :].T + dot(dxt[...], hot, 1, 0)
                val = val.astype(BF16)
                for d in range(8):
                    dst[i, slab(d), :, pl.ds(at, block)] = val[d * 16:(d + 1) * 16]
                return carry

            lax.fori_loop(0, width // block, piece, 0)

    def emb_finish(i):
        fa[i] = reda.last(i).astype(BF16)
        fb[i] = redb.last(i).astype(BF16)

    def put(i):
        for cp in zcopy(i):
            cp.wait_recv()
        for part, mine, other in ((0, fa, za), (1, fb, zb)):
            off = (2 * i + part) * width
            emb_out[:, pl.ds(pl.multiple_of(pp * half + off, 128), width)] = mine[i]
            emb_out[:, pl.ds(pl.multiple_of((1 - pp) * half + off, 128), width)] = other[i]

    def emb_step(k, carry):
        def stage(lag, fn):
            @pl.when((k >= lag) & (k < pairs + lag))
            def _():
                fn(k - lag)

        def late(lag, fn):
            for n in range(2):
                at = 2 * (k - lag) + n

                @pl.when((pp == 0) & (at >= 0) & (at < layers))
                def _():
                    fn(layers - 1 - at)

        late(1, start2)
        stage(1, lambda i: (reda.copy0(i).start(), redb.copy0(i).start()))
        stage(2, lambda i: (reda.copy1(i).start(), redb.copy1(i).start()))
        stage(4, lambda i: (reda.copy2(i).start(), redb.copy2(i).start()))
        stage(6, lambda i: [cp.start() for cp in zcopy(i)])
        stage(0, build)
        late(0, add1)
        stage(1, lambda i: (reda.add0(i), redb.add0(i)))
        stage(3, lambda i: (reda.add1(i), redb.add1(i)))
        stage(5, emb_finish)
        late(4, finish)
        stage(8, put)
        return carry

    lax.fori_loop(0, pairs + 9, emb_step, 0)

    def drain_layer(i, carry):
        red1.drain(i)
        red2.drain(i)
        return carry

    lax.fori_loop(0, layers, drain_layer, 0)

    def drain_pair(i, carry):
        reda.drain(i)
        redb.drain(i)
        for cp in zcopy(i):
            cp.wait_send()
        return carry

    lax.fori_loop(0, pairs, drain_pair, 0)


def fused(tok_ids, d_out, stored_x, w_in, w_out, acc_in, acc_out, acc_emb):
    layers, hid, ff = w_in.shape
    tokens = d_out.shape[1]
    vocab = acc_emb.shape[0]
    pairs, width = 10, 768
    half = 2 * pairs * width
    n1, n2 = hid // 8, ff // 8

    def side(count, *shape):
        return [pltpu.VMEM((count, 8, *shape), BF16), pltpu.VMEM((count, 4, *shape), BF16),
                pltpu.VMEM((count, 2, *shape), BF16), pltpu.VMEM((count, *shape), BF16)]

    piece = pltpu.VMEM((pairs, n1, width), BF16)
    return pl.pallas_call(
        functools.partial(fused_kernel, layers, pairs, width, vocab),
        out_shape=(jax.ShapeDtypeStruct((layers, n1, ff), F32), jax.ShapeDtypeStruct((layers, n2, hid), F32),
                   jax.ShapeDtypeStruct((n1, 2 * half), BF16)),
        in_specs=[VM, ANY, ANY, ANY, ANY, ANY, ANY, ANY],
        out_specs=(VM, VM, VM),
        scratch_shapes=[
            pltpu.VMEM((layers, hid, ff), BF16),
            pltpu.VMEM((layers, ff, hid), BF16),
            pltpu.VMEM((layers + 1, tokens, hid), BF16),
            pltpu.VMEM((layers, tokens, ff), BF16),
            pltpu.VMEM((layers, tokens, ff), F32),
            pltpu.VMEM((layers + 1, tokens, hid), BF16),
            pltpu.VMEM((tokens, ff), BF16),
            pltpu.VMEM((layers, hid, ff), F32),
            pltpu.VMEM((layers, hid, ff), F32),
            pltpu.VMEM((layers, ff, hid), F32),
            pltpu.VMEM((tokens, hid), BF16),
            pltpu.VMEM((2, tokens, hid), BF16),
            *side(layers, n1, ff),
            *side(layers, n2, hid),
            pltpu.VMEM((2 * tokens, 128), jnp.int32),
            pltpu.VMEM((half, hid), F32),
            pltpu.VMEM((hid, 2 * tokens), BF16),
            *side(pairs, n1, width),
            *side(pairs, n1, width),
            piece, piece, piece, piece,
            pltpu.SemaphoreType.DMA((2, layers)),
            pltpu.SemaphoreType.DMA((5,)),
            pltpu.SemaphoreType.DMA((6,)),
            pltpu.SemaphoreType.DMA((6, layers)),
            pltpu.SemaphoreType.DMA((6, layers)),
            pltpu.SemaphoreType.DMA,
            pltpu.SemaphoreType.DMA((6, pairs)),
            pltpu.SemaphoreType.DMA((6, pairs)),
            pltpu.SemaphoreType.DMA((4, pairs)),
        ],
        compiler_params=pltpu.CompilerParams(collective_id=0, has_side_effects=True, vmem_limit_bytes=67043328),
    )(tok_ids, d_out, stored_x, w_in, w_out, acc_in, acc_out, acc_emb)


def mean_kernel(a, b, e, g_in, g_out, g_emb):
    g_in[...] = a[...] * 0.125
    g_out[...] = b[...] * 0.125
    g_emb[...] = e[:, :g_emb.shape[1]].astype(F32) * 0.125


def mean(a, b, e, vocab):
    return pl.pallas_call(
        mean_kernel,
        out_shape=(jax.ShapeDtypeStruct(a.shape, F32), jax.ShapeDtypeStruct(b.shape, F32), jax.ShapeDtypeStruct((e.shape[0], vocab), F32)),
        in_specs=[VM, VM, VM],
        out_specs=(VM, VM, VM),
    )(a, b, e)


def solution(mesh):
    def device_body(tok_ids, d_out, stored_x, w_in, w_out, acc_in, acc_out, acc_emb):
        vocab, hid = acc_emb.shape[1:]
        sums = fused(tok_ids, d_out, stored_x, w_in, w_out, acc_in, acc_out, acc_emb.reshape(vocab, 1, hid))
        grad_in, grad_out, grad_emb = mean(*sums, vocab)
        return grad_in, grad_out, grad_emb.T

    return jax.shard_map(
        device_body,
        mesh=mesh,
        in_specs=(P(None, "dp"), P("pp", "dp", None), P("pp", None, "dp", None), P("pp", None, None), P("pp", None, None),
                  P("pp", "dp", None, None), P("pp", "dp", None, None), P("dp", None, None)),
        out_specs=(P("pp", "dp", None), P("pp", "dp", None), P(None, "dp")),
        check_vma=False,
    )
```

```python
import functools

import jax
import jax.numpy as jnp
from jax import lax
from jax.experimental import pallas as pl
from jax.experimental.pallas import tpu as pltpu
from jax.sharding import PartitionSpec as P

MESH = pl.DeviceIdType.MESH
C0 = 0.7978845608028654
C1 = 0.044715
F32, BF16 = jnp.float32, jnp.bfloat16
ANY = pl.BlockSpec(memory_space=pl.ANY)
VM = pl.BlockSpec(memory_space=pltpu.VMEM)


def coords():
    pp, d = lax.axis_index("pp"), lax.axis_index("dp")
    y, x, c = d // 4, (d // 2) % 2, d % 2
    to_x = {"pp": pp, "dp": d + 2 - 4 * x}
    to_y = {"pp": pp, "dp": d + 4 - 8 * y}
    to_c = {"pp": pp, "dp": d + 1 - 2 * c}
    to_z = {"pp": 1 - pp, "dp": d}
    return pp, y, x, c, to_x, to_y, to_c, to_z


def knock(neighbours):
    barrier = pltpu.get_barrier_semaphore()
    for dev in neighbours:
        pl.semaphore_signal(barrier, inc=1, device_id=dev, device_id_type=MESH)
    return lambda: pl.semaphore_wait(barrier, len(neighbours))


def remote(src, dst, send, recv, dev):
    return pltpu.make_async_remote_copy(src_ref=src, dst_ref=dst, send_sem=send, recv_sem=recv, device_id=dev, device_id_type=MESH)


def slab_xy(d):
    return (d % 2) * 4 + ((d // 2) % 2) * 2 + d // 4


def slab_yx(d):
    return (d % 2) * 4 + (d // 4) * 2 + (d // 2) % 2


class Reduce:
    def __init__(self, src, r0, r1, r2, sems, to, c, p, q):
        self.src, self.r0, self.r1, self.r2, self.sems, self.to = src, r0, r1, r2, sems, to
        self.c, self.p, self.q = c, p, q

    def copy0(self, i):
        return remote(self.src.at[i, pl.ds(4 * (1 - self.c), 4)], self.r0.at[i], self.sems.at[0, i], self.sems.at[1, i], self.to[0])

    def copy1(self, i):
        at = 4 * self.c + 2 * (1 - self.p)
        return remote(self.src.at[i, pl.ds(at, 2)], self.r1.at[i], self.sems.at[2, i], self.sems.at[3, i], self.to[1])

    def copy2(self, i):
        at = 4 * self.c + 2 * self.p + 1 - self.q
        return remote(self.src.at[i, at], self.r2.at[i], self.sems.at[4, i], self.sems.at[5, i], self.to[2])

    def add0(self, i):
        self.copy0(i).wait_recv()
        for k in range(4):
            at = 4 * self.c + k
            self.src[i, at] = (self.src[i, at].astype(F32) + self.r0[i, k].astype(F32)).astype(BF16)

    def add1(self, i):
        self.copy1(i).wait_recv()
        for k in range(2):
            at = 4 * self.c + 2 * self.p + k
            self.src[i, at] = (self.src[i, at].astype(F32) + self.r1[i, k].astype(F32)).astype(BF16)

    def last(self, i):
        self.copy2(i).wait_recv()
        at = 4 * self.c + 2 * self.p + self.q
        return self.src[i, at].astype(F32) + self.r2[i].astype(F32)

    def drain(self, i):
        self.copy0(i).wait_send()
        self.copy1(i).wait_send()
        self.copy2(i).wait_send()


def dot(a, b, ca, cb):
    return lax.dot_general(a, b, (((ca,), (cb,)), ((), ())), preferred_element_type=F32)


def fused_kernel(layers, pairs, width, vocab, tok_ids, d_out, x_in, w_in, w_out, acc_in, acc_out, acc_emb, g_in, g_out, emb_out,
                 w1, w2, xs, hid, slope, gs, dh, dw1, dw2, acc2, cot_in, dxs, s1, s1a, s1b, s1c, s2, s2a, s2b, s2c,
                 rel, buf, dxt, sa, sa0, sa1, sa2, sb, sb0, sb1, sb2, fa, fb, za, zb,
                 wsem, asem, zsem, sem1, sem2, esem, sema, semb, fsem):
    pp, y, x, c, to_x, to_y, to_c, to_z = coords()
    tokens = dxs.shape[1]
    half = 2 * pairs * width
    block = width

    def load(i):
        return (pltpu.make_async_copy(w_in.at[i], w1.at[i], wsem.at[0, i]),
                pltpu.make_async_copy(w_out.at[i], w2.at[i], wsem.at[1, i]))

    def load_emb(act):
        def one(size, base):
            act(pltpu.make_async_copy(acc_emb.at[pl.ds(base, size), 0, :], buf.at[pl.ds(0, size)], esem))

        @pl.when(pp == 0)
        def _():
            one(half, 0)

        @pl.when(pp == 1)
        def _():
            one(vocab - half, half)

    load_x = pltpu.make_async_copy(x_in.at[0, 1 - pp], xs.at[0], asem.at[2])
    load_g = pltpu.make_async_copy(d_out.at[0], gs.at[layers], asem.at[3])
    load_acc1 = pltpu.make_async_copy(acc_in.at[:, 0], dw1, asem.at[0])
    load_acc2 = pltpu.make_async_copy(acc_out.at[:, 0], acc2, asem.at[1])
    enter = knock((to_x, to_y, to_c, to_z))
    load_x.start()
    for i in range(layers):
        for cp in load(i):
            cp.start()

    lane = lax.broadcasted_iota(jnp.int32, (128, 128), 1)
    for j in range(2):
        for b in range(tokens // 128):
            ids = tok_ids[j:j + 1, b * 128:(b + 1) * 128].astype(F32)
            ids = jnp.broadcast_to(ids, (128, 128)).T.astype(jnp.int32)
            rel[pl.ds(j * tokens + b * 128, 128)] = ids - lane
    load_x.wait()

    red1 = Reduce(s1, s1a, s1b, s1c, sem1, (to_c, to_x, to_y), c, x, y)
    red2 = Reduce(s2, s2a, s2b, s2c, sem2, (to_c, to_y, to_x), c, y, x)
    reda = Reduce(sa, sa0, sa1, sa2, sema, (to_c, to_x, to_y), c, x, y)
    redb = Reduce(sb, sb0, sb1, sb2, semb, (to_c, to_y, to_x), c, y, x)

    def forward(lo, hi):
        def body(i, carry):
            xc = xs[i]
            h = dot(xc, w1[i], 1, 0).astype(BF16).astype(F32)
            h2 = h * h
            t = jnp.tanh(h * (C0 + (C0 * C1) * h2))
            cdf = 0.5 + 0.5 * t
            a = (h * cdf).astype(BF16)
            hid[i] = a
            slope[i] = cdf + h * ((cdf * (1.0 - cdf)) * (2.0 * C0 + (6.0 * C0 * C1) * h2))
            xs[i + 1] = (xc.astype(F32) + dot(a, w2[i], 1, 0)).astype(BF16)
            return carry

        lax.fori_loop(lo, hi, body, 0, unroll=3)

    def block_backward(i, first, final):
        gc = gs[i + 1]
        da = dot(gc, w2[i], 1, 1).astype(BF16).astype(F32)
        dhc = (da * slope[i]).astype(BF16)
        dh[...] = dhc
        gs[i] = (gc.astype(F32) + dot(dhc, w1[i], 1, 1)).astype(BF16)
        new2 = dot(gs[i + 1], hid[i], 0, 0)
        if not first:
            new2 = new2 + dw2[i]
        new1 = dot(xs[i], dh[...], 0, 0) + dw1[i]
        if not final:
            dw1[i] = new1
            dw2[i] = new2
            return
        new1 = new1.astype(BF16)
        n1 = new1.shape[0] // 8
        for d in range(8):
            s1[i, slab_xy(d)] = new1[d * n1:(d + 1) * n1]
        new2 = (new2.T + acc2[i]).astype(BF16)
        n2 = new2.shape[0] // 8
        for d in range(8):
            s2[i, slab_yx(d)] = new2[d * n2:(d + 1) * n2]

    def start0(i):
        red1.copy0(i).start()
        red2.copy0(i).start()

    def start1(i):
        red1.copy1(i).start()
        red2.copy1(i).start()

    def start2(i):
        red1.copy2(i).start()
        red2.copy2(i).start()

    def add0(i):
        red1.add0(i)
        red2.add0(i)

    def add1(i):
        red1.add1(i)
        red2.add1(i)

    def finish(i):
        g_in[i] = red1.last(i)
        g_out[i] = red2.last(i)

    def when_layer(k, lag, fn):
        @pl.when((k >= lag) & (k < layers + lag))
        def _():
            fn(layers - 1 - (k - lag))

    send_cot = remote(gs.at[0], cot_in, zsem.at[0], zsem.at[1], to_z)
    send_dx1 = remote(dxs.at[1], dxs.at[1], zsem.at[2], zsem.at[3], to_z)
    send_dx0 = remote(gs.at[0], dxs.at[0], zsem.at[4], zsem.at[5], to_z)

    next_x = pltpu.make_async_copy(x_in.at[0, 0], dxs.at[0], asem.at[4])
    for lo, hi in ((0, 3), (3, layers)):
        for i in range(lo, hi):
            for cp in load(i):
                cp.wait()
        forward(lo, hi)
        if lo == 0:
            load_g.start()
            load_acc1.start()
            load_acc2.start()
            load_emb(lambda cp: cp.start())
            pl.when(pp == 0)(next_x.start)
    load_acc1.wait()
    load_acc2.wait()
    load_g.wait()
    enter()

    @pl.when(pp == 1)
    def _():
        def step(k, carry):
            @pl.when(k == layers)
            def _():
                send_cot.start()

            when_layer(k, 0, lambda i: (block_backward(i, True, True), start0(i)))
            when_layer(k, 2, lambda i: (add0(i), start1(i)))
            when_layer(k, 5, lambda i: (add1(i), start2(i)))
            when_layer(k, 8, finish)
            return carry

        lax.fori_loop(0, layers + 9, step, 0)
        send_cot.wait_send()
        send_dx1.wait_recv()
        dxt[:, pl.ds(tokens, tokens)] = dxs[1].T
        send_dx0.wait_recv()
        dxt[:, pl.ds(0, tokens)] = dxs[0].T

    @pl.when(pp == 0)
    def _():
        def back(k, carry):
            block_backward(layers - 1 - k, True, False)
            return carry

        lax.fori_loop(0, layers, back, 0, unroll=3)
        dxs[1] = gs[0]
        send_dx1.start()
        next_x.wait()
        xs[0] = dxs[0]
        forward(0, layers)
        dxt[:, pl.ds(tokens, tokens)] = dxs[1].T
        send_cot.wait_recv()
        gs[layers] = cot_in[...]

        def step(k, carry):
            @pl.when(k == layers)
            def _():
                send_dx0.start()

            when_layer(k, 0, lambda i: (block_backward(i, False, True), start0(i)))
            when_layer(k, 2, lambda i: (add0(i), start1(i)))
            return carry

        lax.fori_loop(0, layers + 2, step, 0)
        dxt[:, pl.ds(0, tokens)] = gs[0].T
        send_dx1.wait_send()
        send_dx0.wait_send()

    load_emb(lambda cp: cp.wait())

    def zcopy(i):
        return (remote(fa.at[i], za.at[i], fsem.at[0, i], fsem.at[1, i], to_z),
                remote(fb.at[i], zb.at[i], fsem.at[2, i], fsem.at[3, i], to_z))

    def build(i):
        for part, dst, slab in ((0, sa, slab_xy), (1, sb, slab_yx)):
            def piece(j, carry):
                at = pl.multiple_of(j * block, block)
                row = pl.multiple_of((2 * i + part) * width + j * block, block)
                base = pp * half + row
                ids = rel[...]
                hot = jnp.concatenate([jnp.where(ids == base + 128 * n, 1.0, 0.0).astype(BF16) for n in range(block // 128)], axis=1)
                val = buf[pl.ds(row, block), :].T + dot(dxt[...], hot, 1, 0)
                val = val.astype(BF16)
                for d in range(8):
                    dst[i, slab(d), :, pl.ds(at, block)] = val[d * 16:(d + 1) * 16]
                return carry

            lax.fori_loop(0, width // block, piece, 0)

    def emb_finish(i):
        fa[i] = reda.last(i).astype(BF16)
        fb[i] = redb.last(i).astype(BF16)

    def put(i):
        for cp in zcopy(i):
            cp.wait_recv()
        for part, mine, other in ((0, fa, za), (1, fb, zb)):
            off = (2 * i + part) * width
            emb_out[:, pl.ds(pl.multiple_of(pp * half + off, 128), width)] = mine[i]
            emb_out[:, pl.ds(pl.multiple_of((1 - pp) * half + off, 128), width)] = other[i]

    def emb_step(k, carry):
        def stage(lag, fn):
            @pl.when((k >= lag) & (k < pairs + lag))
            def _():
                fn(k - lag)

        def late(lag, fn):
            for n in range(2):
                at = 2 * (k - lag) + n

                @pl.when((pp == 0) & (at >= 0) & (at < layers))
                def _():
                    fn(layers - 1 - at)

        stage(0, lambda i: (build(i), reda.copy0(i).start(), redb.copy0(i).start()))
        late(0, lambda i: (add1(i), start2(i)))
        stage(1, lambda i: (reda.add0(i), redb.add0(i), reda.copy1(i).start(), redb.copy1(i).start()))
        stage(3, lambda i: (reda.add1(i), redb.add1(i), reda.copy2(i).start(), redb.copy2(i).start()))
        stage(5, lambda i: (emb_finish(i), [cp.start() for cp in zcopy(i)]))
        late(4, finish)
        stage(7, put)
        return carry

    lax.fori_loop(0, pairs + 8, emb_step, 0)

    def drain_layer(i, carry):
        red1.drain(i)
        red2.drain(i)
        return carry

    lax.fori_loop(0, layers, drain_layer, 0)

    def drain_pair(i, carry):
        reda.drain(i)
        redb.drain(i)
        for cp in zcopy(i):
            cp.wait_send()
        return carry

    lax.fori_loop(0, pairs, drain_pair, 0)


def fused(tok_ids, d_out, stored_x, w_in, w_out, acc_in, acc_out, acc_emb):
    layers, hid, ff = w_in.shape
    tokens = d_out.shape[1]
    vocab = acc_emb.shape[0]
    pairs, width = 10, 768
    half = 2 * pairs * width
    n1, n2 = hid // 8, ff // 8

    def side(count, *shape):
        return [pltpu.VMEM((count, 8, *shape), BF16), pltpu.VMEM((count, 4, *shape), BF16),
                pltpu.VMEM((count, 2, *shape), BF16), pltpu.VMEM((count, *shape), BF16)]

    piece = pltpu.VMEM((pairs, n1, width), BF16)
    return pl.pallas_call(
        functools.partial(fused_kernel, layers, pairs, width, vocab),
        out_shape=(jax.ShapeDtypeStruct((layers, n1, ff), F32), jax.ShapeDtypeStruct((layers, n2, hid), F32),
                   jax.ShapeDtypeStruct((n1, 2 * half), BF16)),
        in_specs=[VM, ANY, ANY, ANY, ANY, ANY, ANY, ANY],
        out_specs=(VM, VM, VM),
        scratch_shapes=[
            pltpu.VMEM((layers, hid, ff), BF16),
            pltpu.VMEM((layers, ff, hid), BF16),
            pltpu.VMEM((layers + 1, tokens, hid), BF16),
            pltpu.VMEM((layers, tokens, ff), BF16),
            pltpu.VMEM((layers, tokens, ff), F32),
            pltpu.VMEM((layers + 1, tokens, hid), BF16),
            pltpu.VMEM((tokens, ff), BF16),
            pltpu.VMEM((layers, hid, ff), F32),
            pltpu.VMEM((layers, hid, ff), F32),
            pltpu.VMEM((layers, ff, hid), F32),
            pltpu.VMEM((tokens, hid), BF16),
            pltpu.VMEM((2, tokens, hid), BF16),
            *side(layers, n1, ff),
            *side(layers, n2, hid),
            pltpu.VMEM((2 * tokens, 128), jnp.int32),
            pltpu.VMEM((half, hid), F32),
            pltpu.VMEM((hid, 2 * tokens), BF16),
            *side(pairs, n1, width),
            *side(pairs, n1, width),
            piece, piece, piece, piece,
            pltpu.SemaphoreType.DMA((2, layers)),
            pltpu.SemaphoreType.DMA((5,)),
            pltpu.SemaphoreType.DMA((6,)),
            pltpu.SemaphoreType.DMA((6, layers)),
            pltpu.SemaphoreType.DMA((6, layers)),
            pltpu.SemaphoreType.DMA,
            pltpu.SemaphoreType.DMA((6, pairs)),
            pltpu.SemaphoreType.DMA((6, pairs)),
            pltpu.SemaphoreType.DMA((4, pairs)),
        ],
        compiler_params=pltpu.CompilerParams(collective_id=0, has_side_effects=True, vmem_limit_bytes=67043328),
    )(tok_ids, d_out, stored_x, w_in, w_out, acc_in, acc_out, acc_emb)


def mean_kernel(a, b, e, g_in, g_out, g_emb):
    g_in[...] = a[...] * 0.125
    g_out[...] = b[...] * 0.125
    g_emb[...] = e[:, :g_emb.shape[1]].astype(F32) * 0.125


def mean(a, b, e, vocab):
    return pl.pallas_call(
        mean_kernel,
        out_shape=(jax.ShapeDtypeStruct(a.shape, F32), jax.ShapeDtypeStruct(b.shape, F32), jax.ShapeDtypeStruct((e.shape[0], vocab), F32)),
        in_specs=[VM, VM, VM],
        out_specs=(VM, VM, VM),
    )(a, b, e)


def solution(mesh):
    def device_body(tok_ids, d_out, stored_x, w_in, w_out, acc_in, acc_out, acc_emb):
        vocab, hid = acc_emb.shape[1:]
        sums = fused(tok_ids, d_out, stored_x, w_in, w_out, acc_in, acc_out, acc_emb.reshape(vocab, 1, hid))
        grad_in, grad_out, grad_emb = mean(*sums, vocab)
        return grad_in, grad_out, grad_emb.T

    return jax.shard_map(
        device_body,
        mesh=mesh,
        in_specs=(P(None, "dp"), P("pp", "dp", None), P("pp", None, "dp", None), P("pp", None, None), P("pp", None, None),
                  P("pp", "dp", None, None), P("pp", "dp", None, None), P("dp", None, None)),
        out_specs=(P("pp", "dp", None), P("pp", "dp", None), P(None, "dp")),
        check_vma=False,
    )
```

```python
import functools

import jax
import jax.numpy as jnp
from jax import lax
from jax.experimental import pallas as pl
from jax.experimental.pallas import tpu as pltpu
from jax.sharding import PartitionSpec as P

MESH = pl.DeviceIdType.MESH
C0 = 0.7978845608028654
C1 = 0.044715
F32, BF16 = jnp.float32, jnp.bfloat16
ANY = pl.BlockSpec(memory_space=pl.ANY)
VM = pl.BlockSpec(memory_space=pltpu.VMEM)


def coords():
    pp, d = lax.axis_index("pp"), lax.axis_index("dp")
    y, x, c = d // 4, (d // 2) % 2, d % 2
    to_x = {"pp": pp, "dp": d + 2 - 4 * x}
    to_y = {"pp": pp, "dp": d + 4 - 8 * y}
    to_c = {"pp": pp, "dp": d + 1 - 2 * c}
    to_z = {"pp": 1 - pp, "dp": d}
    return pp, y, x, c, to_x, to_y, to_c, to_z


def knock(neighbours):
    barrier = pltpu.get_barrier_semaphore()
    for dev in neighbours:
        pl.semaphore_signal(barrier, inc=1, device_id=dev, device_id_type=MESH)
    return lambda: pl.semaphore_wait(barrier, len(neighbours))


def remote(src, dst, send, recv, dev):
    return pltpu.make_async_remote_copy(src_ref=src, dst_ref=dst, send_sem=send, recv_sem=recv, device_id=dev, device_id_type=MESH)


def slab_xy(d):
    return (d % 2) * 4 + ((d // 2) % 2) * 2 + d // 4


def slab_yx(d):
    return (d % 2) * 4 + (d // 4) * 2 + (d // 2) % 2


class Reduce:
    def __init__(self, src, r0, r1, r2, sems, to, c, p, q):
        self.src, self.r0, self.r1, self.r2, self.sems, self.to = src, r0, r1, r2, sems, to
        self.c, self.p, self.q = c, p, q

    def copy0(self, i):
        return remote(self.src.at[i, pl.ds(4 * (1 - self.c), 4)], self.r0.at[i], self.sems.at[0, i], self.sems.at[1, i], self.to[0])

    def copy1(self, i):
        at = 4 * self.c + 2 * (1 - self.p)
        return remote(self.src.at[i, pl.ds(at, 2)], self.r1.at[i], self.sems.at[2, i], self.sems.at[3, i], self.to[1])

    def copy2(self, i):
        at = 4 * self.c + 2 * self.p + 1 - self.q
        return remote(self.src.at[i, at], self.r2.at[i], self.sems.at[4, i], self.sems.at[5, i], self.to[2])

    def add0(self, i):
        self.copy0(i).wait_recv()
        for k in range(4):
            at = 4 * self.c + k
            self.src[i, at] = (self.src[i, at].astype(F32) + self.r0[i, k].astype(F32)).astype(BF16)

    def add1(self, i):
        self.copy1(i).wait_recv()
        for k in range(2):
            at = 4 * self.c + 2 * self.p + k
            self.src[i, at] = (self.src[i, at].astype(F32) + self.r1[i, k].astype(F32)).astype(BF16)

    def last(self, i):
        self.copy2(i).wait_recv()
        at = 4 * self.c + 2 * self.p + self.q
        return self.src[i, at].astype(F32) + self.r2[i].astype(F32)

    def drain(self, i):
        self.copy0(i).wait_send()
        self.copy1(i).wait_send()
        self.copy2(i).wait_send()


def dot(a, b, ca, cb):
    return lax.dot_general(a, b, (((ca,), (cb,)), ((), ())), preferred_element_type=F32)


def fused_kernel(layers, pairs, width, vocab, tok_ids, d_out, x_in, w_in, w_out, acc_in, acc_out, acc_emb, g_in, g_out, emb_out,
                 w1, w2, xs, hid, slope, gs, dh, dw1, dw2, acc2, cot_in, dxs, s1, s1a, s1b, s1c, s2, s2a, s2b, s2c,
                 ids_in, rel, buf, dxt, sa, sa0, sa1, sa2, sb, sb0, sb1, sb2, fa, fb, za, zb,
                 wsem, asem, zsem, sem1, sem2, esem, sema, semb, fsem):
    pp, y, x, c, to_x, to_y, to_c, to_z = coords()
    tokens = dxs.shape[1]
    half = 2 * pairs * width
    block = width

    def load(i):
        return (pltpu.make_async_copy(w_in.at[i], w1.at[i], wsem.at[0, i]),
                pltpu.make_async_copy(w_out.at[i], w2.at[i], wsem.at[1, i]))

    def load_emb(act):
        def one(size, base):
            act(pltpu.make_async_copy(acc_emb.at[pl.ds(base, size), 0, :], buf.at[pl.ds(0, size)], esem))

        @pl.when(pp == 0)
        def _():
            one(half, 0)

        @pl.when(pp == 1)
        def _():
            one(vocab - half, half)

    load_x = pltpu.make_async_copy(x_in.at[0, 1 - pp], xs.at[0], asem.at[2])
    load_g = pltpu.make_async_copy(d_out.at[0], gs.at[layers], asem.at[3])
    load_acc1 = pltpu.make_async_copy(acc_in.at[:, 0], dw1, asem.at[0])
    load_acc2 = pltpu.make_async_copy(acc_out.at[:, 0], acc2, asem.at[1])
    enter = knock((to_x, to_y, to_c, to_z))
    load_ids = pltpu.make_async_copy(tok_ids, ids_in, asem.at[5])
    load_x.start()
    for i in range(layers):
        for cp in load(i):
            cp.start()

    load_x.wait()

    red1 = Reduce(s1, s1a, s1b, s1c, sem1, (to_c, to_x, to_y), c, x, y)
    red2 = Reduce(s2, s2a, s2b, s2c, sem2, (to_c, to_y, to_x), c, y, x)
    reda = Reduce(sa, sa0, sa1, sa2, sema, (to_c, to_x, to_y), c, x, y)
    redb = Reduce(sb, sb0, sb1, sb2, semb, (to_c, to_y, to_x), c, y, x)

    def forward(lo, hi):
        def body(i, carry):
            xc = xs[i]
            h = dot(xc, w1[i], 1, 0).astype(BF16).astype(F32)
            h2 = h * h
            t = jnp.tanh(h * (C0 + (C0 * C1) * h2))
            cdf = 0.5 + 0.5 * t
            a = (h * cdf).astype(BF16)
            hid[i] = a
            slope[i] = cdf + h * ((cdf * (1.0 - cdf)) * (2.0 * C0 + (6.0 * C0 * C1) * h2))
            xs[i + 1] = (xc.astype(F32) + dot(a, w2[i], 1, 0)).astype(BF16)
            return carry

        lax.fori_loop(lo, hi, body, 0, unroll=3)

    def block_backward(i, first, final):
        gc = gs[i + 1]
        da = dot(gc, w2[i], 1, 1).astype(BF16).astype(F32)
        dhc = (da * slope[i]).astype(BF16)
        dh[...] = dhc
        gs[i] = (gc.astype(F32) + dot(dhc, w1[i], 1, 1)).astype(BF16)
        new2 = dot(gs[i + 1], hid[i], 0, 0)
        if not first:
            new2 = new2 + dw2[i]
        new1 = dot(xs[i], dh[...], 0, 0) + dw1[i]
        if not final:
            dw1[i] = new1
            dw2[i] = new2
            return
        new1 = new1.astype(BF16)
        n1 = new1.shape[0] // 8
        for d in range(8):
            s1[i, slab_xy(d)] = new1[d * n1:(d + 1) * n1]
        new2 = (new2.T + acc2[i]).astype(BF16)
        n2 = new2.shape[0] // 8
        for d in range(8):
            s2[i, slab_yx(d)] = new2[d * n2:(d + 1) * n2]

    def start0(i):
        red1.copy0(i).start()
        red2.copy0(i).start()

    def start1(i):
        red1.copy1(i).start()
        red2.copy1(i).start()

    def start2(i):
        red1.copy2(i).start()
        red2.copy2(i).start()

    def add0(i):
        red1.add0(i)
        red2.add0(i)

    def add1(i):
        red1.add1(i)
        red2.add1(i)

    def finish(i):
        g_in[i] = red1.last(i)
        g_out[i] = red2.last(i)

    group = 2
    groups = layers // group

    def when_group(k, lag, *fns):
        @pl.when((k >= lag) & (k < groups + lag))
        def _():
            for fn in fns:
                for n in range(group):
                    fn(layers - 1 - (k - lag) * group - n)

    send_cot = remote(gs.at[0], cot_in, zsem.at[0], zsem.at[1], to_z)
    send_dx1 = remote(dxs.at[1], dxs.at[1], zsem.at[2], zsem.at[3], to_z)
    send_dx0 = remote(gs.at[0], dxs.at[0], zsem.at[4], zsem.at[5], to_z)

    next_x = pltpu.make_async_copy(x_in.at[0, 0], dxs.at[0], asem.at[4])
    for lo, hi in ((0, 3), (3, layers)):
        for i in range(lo, hi):
            for cp in load(i):
                cp.wait()
        forward(lo, hi)
        if lo == 0:
            load_g.start()
            load_acc1.start()
            load_acc2.start()
            load_ids.start()
            load_emb(lambda cp: cp.start())
            pl.when(pp == 0)(next_x.start)
    load_acc1.wait()
    load_acc2.wait()
    load_g.wait()
    load_ids.wait()
    lane = lax.broadcasted_iota(jnp.int32, (128, 128), 1)
    for j in range(2):
        for b in range(tokens // 128):
            ids = ids_in[j:j + 1, b * 128:(b + 1) * 128].astype(F32)
            ids = jnp.broadcast_to(ids, (128, 128)).T.astype(jnp.int32)
            rel[pl.ds(j * tokens + b * 128, 128)] = ids - lane
    enter()

    @pl.when(pp == 1)
    def _():
        def step(k, carry):
            @pl.when(k == groups)
            def _():
                send_cot.start()

            when_group(k, 0, lambda i: block_backward(i, True, True), start0)
            when_group(k, 1, add0, start1)
            when_group(k, 4, add1, start2)
            when_group(k, 7, finish)
            return carry

        lax.fori_loop(0, groups + 8, step, 0)
        send_dx1.wait_recv()
        dxt[:, pl.ds(tokens, tokens)] = dxs[1].T
        send_dx0.wait_recv()
        dxt[:, pl.ds(0, tokens)] = dxs[0].T

    @pl.when(pp == 0)
    def _():
        def back(k, carry):
            block_backward(layers - 1 - k, True, False)
            return carry

        lax.fori_loop(0, layers, back, 0, unroll=3)
        dxs[1] = gs[0]
        send_dx1.start()
        next_x.wait()
        xs[0] = dxs[0]
        forward(0, layers)
        dxt[:, pl.ds(tokens, tokens)] = dxs[1].T
        send_cot.wait_recv()
        gs[layers] = cot_in[...]

        def step(k, carry):
            @pl.when(k == groups)
            def _():
                send_dx0.start()

            when_group(k, 0, lambda i: block_backward(i, False, True), start0)
            when_group(k, 1, add0, start1)
            return carry

        lax.fori_loop(0, groups + 1, step, 0)
        dxt[:, pl.ds(0, tokens)] = gs[0].T

    load_emb(lambda cp: cp.wait())

    def zcopy(i):
        return (remote(fa.at[i], za.at[i], fsem.at[0, i], fsem.at[1, i], to_z),
                remote(fb.at[i], zb.at[i], fsem.at[2, i], fsem.at[3, i], to_z))

    def build(i):
        for part, dst, slab in ((0, sa, slab_xy), (1, sb, slab_yx)):
            def piece(j, carry):
                at = pl.multiple_of(j * block, block)
                row = pl.multiple_of((2 * i + part) * width + j * block, block)
                base = pp * half + row
                ids = rel[...]
                hot = jnp.concatenate([jnp.where(ids == base + 128 * n, 1.0, 0.0).astype(BF16) for n in range(block // 128)], axis=1)
                val = buf[pl.ds(row, block), :].T + dot(dxt[...], hot, 1, 0)
                val = val.astype(BF16)
                for d in range(8):
                    dst[i, slab(d), :, pl.ds(at, block)] = val[d * 16:(d + 1) * 16]
                return carry

            lax.fori_loop(0, width // block, piece, 0)

    def emb_finish(i):
        fa[i] = reda.last(i).astype(BF16)
        fb[i] = redb.last(i).astype(BF16)

    def put(i):
        for cp in zcopy(i):
            cp.wait_recv()
        for part, mine, other in ((0, fa, za), (1, fb, zb)):
            off = (2 * i + part) * width
            emb_out[:, pl.ds(pl.multiple_of(pp * half + off, 128), width)] = mine[i]
            emb_out[:, pl.ds(pl.multiple_of((1 - pp) * half + off, 128), width)] = other[i]

    def emb_step(k, carry):
        def stage(lag, fn):
            @pl.when((k >= lag) & (k < pairs + lag))
            def _():
                fn(k - lag)

        def late(lag, fn):
            for n in range(2):
                at = 2 * (k - lag) + n

                @pl.when((pp == 0) & (at >= 0) & (at < layers))
                def _():
                    fn(layers - 1 - at)

        stage(0, lambda i: (build(i), reda.copy0(i).start(), redb.copy0(i).start()))
        late(0, lambda i: (add1(i), start2(i)))
        stage(1, lambda i: (reda.add0(i), redb.add0(i), reda.copy1(i).start(), redb.copy1(i).start()))
        stage(3, lambda i: (reda.add1(i), redb.add1(i), reda.copy2(i).start(), redb.copy2(i).start()))
        stage(5, lambda i: (emb_finish(i), [cp.start() for cp in zcopy(i)]))
        late(4, finish)
        stage(7, put)
        return carry

    lax.fori_loop(0, pairs + 8, emb_step, 0)

    @pl.when(pp == 1)
    def _():
        send_cot.wait_send()

    @pl.when(pp == 0)
    def _():
        send_dx1.wait_send()
        send_dx0.wait_send()

    def drain_layer(i, carry):
        red1.drain(i)
        red2.drain(i)
        return carry

    lax.fori_loop(0, layers, drain_layer, 0)

    def drain_pair(i, carry):
        reda.drain(i)
        redb.drain(i)
        for cp in zcopy(i):
            cp.wait_send()
        return carry

    lax.fori_loop(0, pairs, drain_pair, 0)


def fused(tok_ids, d_out, stored_x, w_in, w_out, acc_in, acc_out, acc_emb):
    layers, hid, ff = w_in.shape
    tokens = d_out.shape[1]
    vocab = acc_emb.shape[0]
    pairs, width = 10, 768
    half = 2 * pairs * width
    n1, n2 = hid // 8, ff // 8

    def side(count, *shape):
        return [pltpu.VMEM((count, 8, *shape), BF16), pltpu.VMEM((count, 4, *shape), BF16),
                pltpu.VMEM((count, 2, *shape), BF16), pltpu.VMEM((count, *shape), BF16)]

    piece = pltpu.VMEM((pairs, n1, width), BF16)
    return pl.pallas_call(
        functools.partial(fused_kernel, layers, pairs, width, vocab),
        out_shape=(pltpu.VMEM((layers, n1, ff), F32), pltpu.VMEM((layers, n2, hid), F32), pltpu.VMEM((n1, 2 * half), BF16)),
        in_specs=[ANY, ANY, ANY, ANY, ANY, ANY, ANY, ANY],
        out_specs=(VM, VM, VM),
        scratch_shapes=[
            pltpu.VMEM((layers, hid, ff), BF16),
            pltpu.VMEM((layers, ff, hid), BF16),
            pltpu.VMEM((layers + 1, tokens, hid), BF16),
            pltpu.VMEM((layers, tokens, ff), BF16),
            pltpu.VMEM((layers, tokens, ff), F32),
            pltpu.VMEM((layers + 1, tokens, hid), BF16),
            pltpu.VMEM((tokens, ff), BF16),
            pltpu.VMEM((layers, hid, ff), F32),
            pltpu.VMEM((layers, hid, ff), F32),
            pltpu.VMEM((layers, ff, hid), F32),
            pltpu.VMEM((tokens, hid), BF16),
            pltpu.VMEM((2, tokens, hid), BF16),
            *side(layers, n1, ff),
            *side(layers, n2, hid),
            pltpu.VMEM((2, tokens), jnp.int32),
            pltpu.VMEM((2 * tokens, 128), jnp.int32),
            pltpu.VMEM((half, hid), F32),
            pltpu.VMEM((hid, 2 * tokens), BF16),
            *side(pairs, n1, width),
            *side(pairs, n1, width),
            piece, piece, piece, piece,
            pltpu.SemaphoreType.DMA((2, layers)),
            pltpu.SemaphoreType.DMA((6,)),
            pltpu.SemaphoreType.DMA((6,)),
            pltpu.SemaphoreType.DMA((6, layers)),
            pltpu.SemaphoreType.DMA((6, layers)),
            pltpu.SemaphoreType.DMA,
            pltpu.SemaphoreType.DMA((6, pairs)),
            pltpu.SemaphoreType.DMA((6, pairs)),
            pltpu.SemaphoreType.DMA((4, pairs)),
        ],
        compiler_params=pltpu.CompilerParams(collective_id=0, has_side_effects=True, vmem_limit_bytes=65 * 10**6),
    )(tok_ids, d_out, stored_x, w_in, w_out, acc_in, acc_out, acc_emb)


def mean_kernel(a, b, e, g_in, g_out, g_emb):
    g_in[...] = a[...] * 0.125
    g_out[...] = b[...] * 0.125
    g_emb[...] = e[:, :g_emb.shape[1]].astype(F32) * 0.125


def mean(a, b, e, vocab):
    return pl.pallas_call(
        mean_kernel,
        out_shape=(jax.ShapeDtypeStruct(a.shape, F32), jax.ShapeDtypeStruct(b.shape, F32), jax.ShapeDtypeStruct((e.shape[0], vocab), F32)),
        in_specs=[VM, VM, VM],
        out_specs=(VM, VM, VM),
        compiler_params=pltpu.CompilerParams(vmem_limit_bytes=8 * 2**20),
    )(a, b, e)


def solution(mesh):
    def device_body(tok_ids, d_out, stored_x, w_in, w_out, acc_in, acc_out, acc_emb):
        vocab, hid = acc_emb.shape[1:]
        sums = fused(tok_ids, d_out, stored_x, w_in, w_out, acc_in, acc_out, acc_emb.reshape(vocab, 1, hid))
        grad_in, grad_out, grad_emb = mean(*sums, vocab)
        return grad_in, grad_out, grad_emb.T

    return jax.shard_map(
        device_body,
        mesh=mesh,
        in_specs=(P(None, "dp"), P("pp", "dp", None), P("pp", None, "dp", None), P("pp", None, None), P("pp", None, None),
                  P("pp", "dp", None, None), P("pp", "dp", None, None), P("dp", None, None)),
        out_specs=(P("pp", "dp", None), P("pp", "dp", None), P(None, "dp")),
        check_vma=False,
    )
```

```python
import functools

import jax
import jax.numpy as jnp
from jax import lax
from jax.experimental import pallas as pl
from jax.experimental.pallas import tpu as pltpu
from jax.sharding import PartitionSpec as P

MESH = pl.DeviceIdType.MESH
C0 = 0.7978845608028654
C1 = 0.044715
F32, BF16 = jnp.float32, jnp.bfloat16
ANY = pl.BlockSpec(memory_space=pl.ANY)
VM = pl.BlockSpec(memory_space=pltpu.VMEM)


def coords():
    pp, d = lax.axis_index("pp"), lax.axis_index("dp")
    y, x, c = d // 4, (d // 2) % 2, d % 2
    to_x = {"pp": pp, "dp": d + 2 - 4 * x}
    to_y = {"pp": pp, "dp": d + 4 - 8 * y}
    to_c = {"pp": pp, "dp": d + 1 - 2 * c}
    to_z = {"pp": 1 - pp, "dp": d}
    return pp, y, x, c, to_x, to_y, to_c, to_z


def knock(neighbours):
    barrier = pltpu.get_barrier_semaphore()
    for dev in neighbours:
        pl.semaphore_signal(barrier, inc=1, device_id=dev, device_id_type=MESH)
    return lambda: pl.semaphore_wait(barrier, len(neighbours))


def remote(src, dst, send, recv, dev):
    return pltpu.make_async_remote_copy(src_ref=src, dst_ref=dst, send_sem=send, recv_sem=recv, device_id=dev, device_id_type=MESH)


def slab_xy(d):
    return (d % 2) * 4 + ((d // 2) % 2) * 2 + d // 4


def slab_yx(d):
    return (d % 2) * 4 + (d // 4) * 2 + (d // 2) % 2


class Reduce:
    def __init__(self, src, r0, r1, r2, sems, to, c, p, q):
        self.src, self.r0, self.r1, self.r2, self.sems, self.to = src, r0, r1, r2, sems, to
        self.c, self.p, self.q = c, p, q

    def copy0(self, i):
        return remote(self.src.at[i, pl.ds(4 * (1 - self.c), 4)], self.r0.at[i], self.sems.at[0, i], self.sems.at[1, i], self.to[0])

    def copy1(self, i):
        at = 4 * self.c + 2 * (1 - self.p)
        return remote(self.src.at[i, pl.ds(at, 2)], self.r1.at[i], self.sems.at[2, i], self.sems.at[3, i], self.to[1])

    def copy2(self, i):
        at = 4 * self.c + 2 * self.p + 1 - self.q
        return remote(self.src.at[i, at], self.r2.at[i], self.sems.at[4, i], self.sems.at[5, i], self.to[2])

    def add0(self, i):
        self.copy0(i).wait_recv()
        for k in range(4):
            at = 4 * self.c + k
            self.src[i, at] = (self.src[i, at].astype(F32) + self.r0[i, k].astype(F32)).astype(BF16)

    def add1(self, i):
        self.copy1(i).wait_recv()
        for k in range(2):
            at = 4 * self.c + 2 * self.p + k
            self.src[i, at] = (self.src[i, at].astype(F32) + self.r1[i, k].astype(F32)).astype(BF16)

    def last(self, i):
        self.copy2(i).wait_recv()
        at = 4 * self.c + 2 * self.p + self.q
        return self.src[i, at].astype(F32) + self.r2[i].astype(F32)

    def drain(self, i):
        self.copy0(i).wait_send()
        self.copy1(i).wait_send()
        self.copy2(i).wait_send()


def dot(a, b, ca, cb):
    return lax.dot_general(a, b, (((ca,), (cb,)), ((), ())), preferred_element_type=F32)


def fused_kernel(layers, pairs, width, vocab, tok_ids, d_out, x_in, w_in, w_out, acc_in, acc_out, acc_emb, g_in, g_out, emb_out,
                 w1, w2, xs, hid, slope, gs, dh, dw1, dw2, acc2, cot_in, dxs, s1, s1a, s1b, s1c, s2, s2a, s2b, s2c,
                 ids_in, rel, buf, dxt, sa, sa0, sa1, sa2, sb, sb0, sb1, sb2, fa, fb, za, zb,
                 wsem, asem, zsem, sem1, sem2, esem, sema, semb, fsem):
    pp, y, x, c, to_x, to_y, to_c, to_z = coords()
    tokens = dxs.shape[1]
    half = 2 * pairs * width
    block = width

    def load(i):
        return (pltpu.make_async_copy(w_in.at[i], w1.at[i], wsem.at[0, i]),
                pltpu.make_async_copy(w_out.at[i], w2.at[i], wsem.at[1, i]))

    def load_emb(act):
        def one(size, base):
            act(pltpu.make_async_copy(acc_emb.at[pl.ds(base, size), 0, :], buf.at[pl.ds(0, size)], esem))

        @pl.when(pp == 0)
        def _():
            one(half, 0)

        @pl.when(pp == 1)
        def _():
            one(vocab - half, half)

    load_x = pltpu.make_async_copy(x_in.at[0, 1 - pp], xs.at[0], asem.at[2])
    load_g = pltpu.make_async_copy(d_out.at[0], gs.at[layers], asem.at[3])
    load_acc1 = pltpu.make_async_copy(acc_in.at[:, 0], dw1, asem.at[0])
    load_acc2 = pltpu.make_async_copy(acc_out.at[:, 0], acc2, asem.at[1])
    enter = knock((to_x, to_y, to_c, to_z))
    load_ids = pltpu.make_async_copy(tok_ids, ids_in, asem.at[5])
    load_x.start()
    for i in range(layers):
        for cp in load(i):
            cp.start()

    load_x.wait()

    red1 = Reduce(s1, s1a, s1b, s1c, sem1, (to_c, to_x, to_y), c, x, y)
    red2 = Reduce(s2, s2a, s2b, s2c, sem2, (to_c, to_y, to_x), c, y, x)
    reda = Reduce(sa, sa0, sa1, sa2, sema, (to_c, to_x, to_y), c, x, y)
    redb = Reduce(sb, sb0, sb1, sb2, semb, (to_c, to_y, to_x), c, y, x)

    def forward(lo, hi):
        def body(i, carry):
            xc = xs[i]
            h = dot(xc, w1[i], 1, 0).astype(BF16).astype(F32)
            h2 = h * h
            t = jnp.tanh(h * (C0 + (C0 * C1) * h2))
            cdf = 0.5 + 0.5 * t
            a = (h * cdf).astype(BF16)
            hid[i] = a
            slope[i] = cdf + h * ((cdf * (1.0 - cdf)) * (2.0 * C0 + (6.0 * C0 * C1) * h2))
            xs[i + 1] = (xc.astype(F32) + dot(a, w2[i], 1, 0)).astype(BF16)
            return carry

        lax.fori_loop(lo, hi, body, 0, unroll=hi - lo)

    def block_backward(i, first, final, then=None):
        gc = gs[i + 1]
        da = dot(gc, w2[i], 1, 1).astype(BF16).astype(F32)
        dhc = (da * slope[i]).astype(BF16)
        dh[...] = dhc
        gs[i] = (gc.astype(F32) + dot(dhc, w1[i], 1, 1)).astype(BF16)
        if then is not None:
            then()
        new2 = dot(gs[i + 1], hid[i], 0, 0)
        if not first:
            new2 = new2 + dw2[i]
        new1 = dot(xs[i], dh[...], 0, 0) + dw1[i]
        if not final:
            dw1[i] = new1
            dw2[i] = new2
            return
        new1 = new1.astype(BF16)
        n1 = new1.shape[0] // 8
        for d in range(8):
            s1[i, slab_xy(d)] = new1[d * n1:(d + 1) * n1]
        new2 = (new2.T + acc2[i]).astype(BF16)
        n2 = new2.shape[0] // 8
        for d in range(8):
            s2[i, slab_yx(d)] = new2[d * n2:(d + 1) * n2]

    def start0(i):
        red1.copy0(i).start()
        red2.copy0(i).start()

    def start1(i):
        red1.copy1(i).start()
        red2.copy1(i).start()

    def start2(i):
        red1.copy2(i).start()
        red2.copy2(i).start()

    def add0(i):
        red1.add0(i)
        red2.add0(i)

    def add1(i):
        red1.add1(i)
        red2.add1(i)

    def finish(i):
        g_in[i] = red1.last(i)
        g_out[i] = red2.last(i)

    def when_layer(k, lag, *fns):
        @pl.when((k >= lag) & (k < layers + lag))
        def _():
            for fn in fns:
                fn(layers - 1 - (k - lag))

    send_cot = remote(gs.at[0], cot_in, zsem.at[0], zsem.at[1], to_z)
    send_dx1 = remote(dxs.at[1], dxs.at[1], zsem.at[2], zsem.at[3], to_z)
    send_dx0 = remote(gs.at[0], dxs.at[0], zsem.at[4], zsem.at[5], to_z)

    next_x = pltpu.make_async_copy(x_in.at[0, 0], dxs.at[0], asem.at[4])
    for lo, hi in ((0, 3), (3, layers)):
        for i in range(lo, hi):
            for cp in load(i):
                cp.wait()
        forward(lo, hi)
        if lo == 0:
            load_g.start()
            load_acc1.start()
            load_acc2.start()
            load_ids.start()
            load_emb(lambda cp: cp.start())
            pl.when(pp == 0)(next_x.start)
    load_acc1.wait()
    load_acc2.wait()
    load_g.wait()
    load_ids.wait()
    lane = lax.broadcasted_iota(jnp.int32, (128, 128), 1)
    for j in range(2):
        for b in range(tokens // 128):
            ids = ids_in[j:j + 1, b * 128:(b + 1) * 128].astype(F32)
            ids = jnp.broadcast_to(ids, (128, 128)).T.astype(jnp.int32)
            rel[pl.ds(j * tokens + b * 128, 128)] = ids - lane
    enter()

    @pl.when(pp == 1)
    def _():
        def last_block(k, carry):
            block_backward(layers - 1 - k, True, True)
            return carry

        def send_block(k, carry):
            start0(layers - 1 - k)
            return carry

        middle = layers // 2
        lax.fori_loop(0, middle, last_block, 0, unroll=3)
        lax.fori_loop(0, middle, send_block, 0)
        lax.fori_loop(middle, layers, last_block, 0, unroll=3)
        send_cot.start()
        lax.fori_loop(middle, layers, send_block, 0)

        def step(k, carry):
            when_layer(k, 0, add0, start1)
            when_layer(k, 3, add1, start2)
            when_layer(k, 6, finish)
            return carry

        lax.fori_loop(0, layers + 6, step, 0)
        send_dx1.wait_recv()
        dxt[:, pl.ds(tokens, tokens)] = dxs[1].T
        send_dx0.wait_recv()
        dxt[:, pl.ds(0, tokens)] = dxs[0].T

    @pl.when(pp == 0)
    def _():
        def back(k, carry):
            block_backward(layers - 1 - k, True, False)
            return carry

        lax.fori_loop(0, layers, back, 0, unroll=layers)
        dxs[1] = gs[0]
        send_dx1.start()
        next_x.wait()
        xs[0] = dxs[0]
        forward(0, layers)
        dxt[:, pl.ds(tokens, tokens)] = dxs[1].T
        send_cot.wait_recv()
        gs[layers] = cot_in[...]

        for i in reversed(range(layers)):
            block_backward(i, False, True, send_dx0.start if i == 0 else None)
            start0(i)
            if i + 2 < layers:
                add0(i + 2)
                start1(i + 2)
        for i in (1, 0):
            add0(i)
            start1(i)
        dxt[:, pl.ds(0, tokens)] = gs[0].T

    load_emb(lambda cp: cp.wait())

    def zcopy(i):
        return (remote(fa.at[i], za.at[i], fsem.at[0, i], fsem.at[1, i], to_z),
                remote(fb.at[i], zb.at[i], fsem.at[2, i], fsem.at[3, i], to_z))

    def build(i):
        for part, dst, slab in ((0, sa, slab_xy), (1, sb, slab_yx)):
            def piece(j, carry):
                at = pl.multiple_of(j * block, block)
                row = pl.multiple_of((2 * i + part) * width + j * block, block)
                base = pp * half + row
                ids = rel[...]
                hot = jnp.concatenate([jnp.where(ids == base + 128 * n, 1.0, 0.0).astype(BF16) for n in range(block // 128)], axis=1)
                val = buf[pl.ds(row, block), :].T + dot(dxt[...], hot, 1, 0)
                val = val.astype(BF16)
                for d in range(8):
                    dst[i, slab(d), :, pl.ds(at, block)] = val[d * 16:(d + 1) * 16]
                return carry

            lax.fori_loop(0, width // block, piece, 0)

    def emb_finish(i):
        fa[i] = reda.last(i).astype(BF16)
        fb[i] = redb.last(i).astype(BF16)

    def put(i):
        for cp in zcopy(i):
            cp.wait_recv()
        for part, mine, other in ((0, fa, za), (1, fb, zb)):
            off = (2 * i + part) * width
            emb_out[:, pl.ds(pl.multiple_of(pp * half + off, 128), width)] = mine[i]
            emb_out[:, pl.ds(pl.multiple_of((1 - pp) * half + off, 128), width)] = other[i]

    def emb_step(k, carry):
        def stage(lag, fn):
            @pl.when((k >= lag) & (k < pairs + lag))
            def _():
                fn(k - lag)

        def late(lag, fn):
            for n in range(2):
                at = 2 * (k - lag) + n

                @pl.when((pp == 0) & (at >= 0) & (at < layers))
                def _():
                    fn(layers - 1 - at)

        stage(0, lambda i: (build(i), reda.copy0(i).start(), redb.copy0(i).start()))
        late(0, lambda i: (add1(i), start2(i)))
        stage(1, lambda i: (reda.add0(i), redb.add0(i), reda.copy1(i).start(), redb.copy1(i).start()))
        stage(3, lambda i: (reda.add1(i), redb.add1(i), reda.copy2(i).start(), redb.copy2(i).start()))
        stage(5, lambda i: (emb_finish(i), [cp.start() for cp in zcopy(i)]))
        late(4, finish)
        stage(7, put)
        return carry

    lax.fori_loop(0, pairs + 8, emb_step, 0)

    @pl.when(pp == 1)
    def _():
        send_cot.wait_send()

    @pl.when(pp == 0)
    def _():
        send_dx1.wait_send()
        send_dx0.wait_send()

    def drain_layer(i, carry):
        red1.drain(i)
        red2.drain(i)
        return carry

    lax.fori_loop(0, layers, drain_layer, 0)

    def drain_pair(i, carry):
        reda.drain(i)
        redb.drain(i)
        for cp in zcopy(i):
            cp.wait_send()
        return carry

    lax.fori_loop(0, pairs, drain_pair, 0)


def fused(tok_ids, d_out, stored_x, w_in, w_out, acc_in, acc_out, acc_emb):
    layers, hid, ff = w_in.shape
    tokens = d_out.shape[1]
    vocab = acc_emb.shape[0]
    pairs, width = 10, 768
    half = 2 * pairs * width
    n1, n2 = hid // 8, ff // 8

    def side(count, *shape):
        return [pltpu.VMEM((count, 8, *shape), BF16), pltpu.VMEM((count, 4, *shape), BF16),
                pltpu.VMEM((count, 2, *shape), BF16), pltpu.VMEM((count, *shape), BF16)]

    piece = pltpu.VMEM((pairs, n1, width), BF16)
    return pl.pallas_call(
        functools.partial(fused_kernel, layers, pairs, width, vocab),
        out_shape=(pltpu.VMEM((layers, n1, ff), F32), pltpu.VMEM((layers, n2, hid), F32), pltpu.VMEM((n1, 2 * half), BF16)),
        in_specs=[ANY, ANY, ANY, ANY, ANY, ANY, ANY, ANY],
        out_specs=(VM, VM, VM),
        scratch_shapes=[
            pltpu.VMEM((layers, hid, ff), BF16),
            pltpu.VMEM((layers, ff, hid), BF16),
            pltpu.VMEM((layers + 1, tokens, hid), BF16),
            pltpu.VMEM((layers, tokens, ff), BF16),
            pltpu.VMEM((layers, tokens, ff), F32),
            pltpu.VMEM((layers + 1, tokens, hid), BF16),
            pltpu.VMEM((tokens, ff), BF16),
            pltpu.VMEM((layers, hid, ff), F32),
            pltpu.VMEM((layers, hid, ff), F32),
            pltpu.VMEM((layers, ff, hid), F32),
            pltpu.VMEM((tokens, hid), BF16),
            pltpu.VMEM((2, tokens, hid), BF16),
            *side(layers, n1, ff),
            *side(layers, n2, hid),
            pltpu.VMEM((2, tokens), jnp.int32),
            pltpu.VMEM((2 * tokens, 128), jnp.int32),
            pltpu.VMEM((half, hid), F32),
            pltpu.VMEM((hid, 2 * tokens), BF16),
            *side(pairs, n1, width),
            *side(pairs, n1, width),
            piece, piece, piece, piece,
            pltpu.SemaphoreType.DMA((2, layers)),
            pltpu.SemaphoreType.DMA((6,)),
            pltpu.SemaphoreType.DMA((6,)),
            pltpu.SemaphoreType.DMA((6, layers)),
            pltpu.SemaphoreType.DMA((6, layers)),
            pltpu.SemaphoreType.DMA,
            pltpu.SemaphoreType.DMA((6, pairs)),
            pltpu.SemaphoreType.DMA((6, pairs)),
            pltpu.SemaphoreType.DMA((4, pairs)),
        ],
        compiler_params=pltpu.CompilerParams(collective_id=0, has_side_effects=True, vmem_limit_bytes=65 * 10**6),
    )(tok_ids, d_out, stored_x, w_in, w_out, acc_in, acc_out, acc_emb)


def mean_kernel(a, b, e, g_in, g_out, g_emb):
    g_in[...] = a[...] * 0.125
    g_out[...] = b[...] * 0.125
    g_emb[...] = e[:, :g_emb.shape[1]].astype(F32) * 0.125


def mean(a, b, e, vocab):
    return pl.pallas_call(
        mean_kernel,
        out_shape=(jax.ShapeDtypeStruct(a.shape, F32), jax.ShapeDtypeStruct(b.shape, F32), jax.ShapeDtypeStruct((e.shape[0], vocab), F32)),
        in_specs=[VM, VM, VM],
        out_specs=(VM, VM, VM),
        compiler_params=pltpu.CompilerParams(vmem_limit_bytes=8 * 2**20),
    )(a, b, e)


def solution(mesh):
    def device_body(tok_ids, d_out, stored_x, w_in, w_out, acc_in, acc_out, acc_emb):
        vocab, hid = acc_emb.shape[1:]
        sums = fused(tok_ids, d_out, stored_x, w_in, w_out, acc_in, acc_out, acc_emb.reshape(vocab, 1, hid))
        grad_in, grad_out, grad_emb = mean(*sums, vocab)
        return grad_in, grad_out, grad_emb.T

    return jax.shard_map(
        device_body,
        mesh=mesh,
        in_specs=(P(None, "dp"), P("pp", "dp", None), P("pp", None, "dp", None), P("pp", None, None), P("pp", None, None),
                  P("pp", "dp", None, None), P("pp", "dp", None, None), P("dp", None, None)),
        out_specs=(P("pp", "dp", None), P("pp", "dp", None), P(None, "dp")),
        check_vma=False,
    )
```

```python
import functools

import jax
import jax.numpy as jnp
from jax import lax
from jax.experimental import pallas as pl
from jax.experimental.pallas import tpu as pltpu
from jax.sharding import PartitionSpec as P

MESH = pl.DeviceIdType.MESH
C0 = 0.7978845608028654
C1 = 0.044715
F32, BF16 = jnp.float32, jnp.bfloat16
ANY = pl.BlockSpec(memory_space=pl.ANY)
VM = pl.BlockSpec(memory_space=pltpu.VMEM)


def coords():
    pp, d = lax.axis_index("pp"), lax.axis_index("dp")
    y, x, c = d // 4, (d // 2) % 2, d % 2
    to_x = {"pp": pp, "dp": d + 2 - 4 * x}
    to_y = {"pp": pp, "dp": d + 4 - 8 * y}
    to_c = {"pp": pp, "dp": d + 1 - 2 * c}
    to_z = {"pp": 1 - pp, "dp": d}
    return pp, y, x, c, to_x, to_y, to_c, to_z


def knock(neighbours):
    barrier = pltpu.get_barrier_semaphore()
    for dev in neighbours:
        pl.semaphore_signal(barrier, inc=1, device_id=dev, device_id_type=MESH)
    return lambda: pl.semaphore_wait(barrier, len(neighbours))


def remote(src, dst, send, recv, dev):
    return pltpu.make_async_remote_copy(src_ref=src, dst_ref=dst, send_sem=send, recv_sem=recv, device_id=dev, device_id_type=MESH)


def slab_xy(d):
    return (d % 2) * 4 + ((d // 2) % 2) * 2 + d // 4


def slab_yx(d):
    return (d % 2) * 4 + (d // 4) * 2 + (d // 2) % 2


class Reduce:
    def __init__(self, src, r0, r1, r2, sems, to, c, p, q):
        self.src, self.r0, self.r1, self.r2, self.sems, self.to = src, r0, r1, r2, sems, to
        self.c, self.p, self.q = c, p, q

    def copy0(self, i):
        return remote(self.src.at[i, pl.ds(4 * (1 - self.c), 4)], self.r0.at[i], self.sems.at[0, i], self.sems.at[1, i], self.to[0])

    def copy1(self, i):
        at = 4 * self.c + 2 * (1 - self.p)
        return remote(self.src.at[i, pl.ds(at, 2)], self.r1.at[i], self.sems.at[2, i], self.sems.at[3, i], self.to[1])

    def copy2(self, i):
        at = 4 * self.c + 2 * self.p + 1 - self.q
        return remote(self.src.at[i, at], self.r2.at[i], self.sems.at[4, i], self.sems.at[5, i], self.to[2])

    def add0(self, i):
        self.copy0(i).wait_recv()
        for k in range(4):
            at = 4 * self.c + k
            self.src[i, at] = (self.src[i, at].astype(F32) + self.r0[i, k].astype(F32)).astype(BF16)

    def add1(self, i):
        self.copy1(i).wait_recv()
        for k in range(2):
            at = 4 * self.c + 2 * self.p + k
            self.src[i, at] = (self.src[i, at].astype(F32) + self.r1[i, k].astype(F32)).astype(BF16)

    def last(self, i):
        self.copy2(i).wait_recv()
        at = 4 * self.c + 2 * self.p + self.q
        return self.src[i, at].astype(F32) + self.r2[i].astype(F32)

    def drain(self, i):
        self.copy0(i).wait_send()
        self.copy1(i).wait_send()
        self.copy2(i).wait_send()


def dot(a, b, ca, cb):
    return lax.dot_general(a, b, (((ca,), (cb,)), ((), ())), preferred_element_type=F32)


def fused_kernel(layers, pairs, split, width, vocab, tok_ids, d_out, x_in, w_in, w_out, acc_in, acc_out, acc_emb, g_in, g_out, emb_out,
                 w1, w2, xs, hid, slope, gs, dh, dw1, dw2, acc2, cot_in, dxs, s1, s1a, s1b, s1c, s2, s2a, s2b, s2c,
                 ids_in, rel, buf, dxt, sa, sa0, sa1, sa2, sb, sb0, sb1, sb2, za, zb,
                 wsem, asem, zsem, sem1, sem2, esem, sema, semb, fsem):
    pp, y, x, c, to_x, to_y, to_c, to_z = coords()
    tokens = dxs.shape[1]
    head = 2 * split * width
    mine, theirs = split + pp * (pairs - split), pairs - pp * (pairs - split)
    my_row, their_row = pp * head, (1 - pp) * head
    block = width

    def load(i):
        return (pltpu.make_async_copy(w_in.at[i], w1.at[i], wsem.at[0, i]),
                pltpu.make_async_copy(w_out.at[i], w2.at[i], wsem.at[1, i]))

    def load_emb(act):
        def one(size, base):
            act(pltpu.make_async_copy(acc_emb.at[pl.ds(base, size), 0, :], buf.at[pl.ds(0, size)], esem))

        @pl.when(pp == 0)
        def _():
            one(head, 0)

        @pl.when(pp == 1)
        def _():
            one(vocab - head, head)

    load_x = pltpu.make_async_copy(x_in.at[0, 1 - pp], xs.at[0], asem.at[2])
    load_g = pltpu.make_async_copy(d_out.at[0], gs.at[layers % 2], asem.at[3])
    load_acc1 = pltpu.make_async_copy(acc_in.at[:, 0], dw1, asem.at[0])
    load_acc2 = pltpu.make_async_copy(acc_out.at[:, 0], acc2, asem.at[1])
    enter = knock((to_x, to_y, to_c, to_z))
    load_ids = pltpu.make_async_copy(tok_ids, ids_in, asem.at[5])
    load_x.start()
    for i in range(layers):
        for cp in load(i):
            cp.start()

    load_x.wait()

    red1 = Reduce(s1, s1a, s1b, s1c, sem1, (to_c, to_x, to_y), c, x, y)
    red2 = Reduce(s2, s2a, s2b, s2c, sem2, (to_c, to_y, to_x), c, y, x)
    reda = Reduce(sa, sa0, sa1, sa2, sema, (to_c, to_x, to_y), c, x, y)
    redb = Reduce(sb, sb0, sb1, sb2, semb, (to_c, to_y, to_x), c, y, x)

    def forward(lo, hi):
        def body(i, carry):
            xc = xs[i]
            h = dot(xc, w1[i], 1, 0).astype(BF16).astype(F32)
            h2 = h * h
            t = jnp.tanh(h * (C0 + (C0 * C1) * h2))
            cdf = 0.5 + 0.5 * t
            a = (h * cdf).astype(BF16)
            hid[i] = a
            slope[i] = cdf + h * ((cdf * (1.0 - cdf)) * (2.0 * C0 + (6.0 * C0 * C1) * h2))
            xs[i + 1] = (xc.astype(F32) + dot(a, w2[i], 1, 0)).astype(BF16)
            return carry

        lax.fori_loop(lo, hi, body, 0, unroll=hi - lo)

    def block_backward(i, first, final, then=None):
        gc = gs[(i + 1) % 2]
        da = dot(gc, w2[i], 1, 1).astype(BF16).astype(F32)
        dhc = (da * slope[i]).astype(BF16)
        dh[...] = dhc
        gs[i % 2] = (gc.astype(F32) + dot(dhc, w1[i], 1, 1)).astype(BF16)
        if then is not None:
            then()
        new2 = dot(gs[(i + 1) % 2], hid[i], 0, 0)
        if not first:
            new2 = new2 + dw2[i]
        new1 = dot(xs[i], dh[...], 0, 0) + dw1[i]
        if not final:
            dw1[i] = new1
            dw2[i] = new2
            return
        new1 = new1.astype(BF16)
        n1 = new1.shape[0] // 8
        for d in range(8):
            s1[i, slab_xy(d)] = new1[d * n1:(d + 1) * n1]
        new2 = (new2.T + acc2[i]).astype(BF16)
        n2 = new2.shape[0] // 8
        for d in range(8):
            s2[i, slab_yx(d)] = new2[d * n2:(d + 1) * n2]

    def start0(i):
        red1.copy0(i).start()
        red2.copy0(i).start()

    def start1(i):
        red1.copy1(i).start()
        red2.copy1(i).start()

    def start2(i):
        red1.copy2(i).start()
        red2.copy2(i).start()

    def add0(i):
        red1.add0(i)
        red2.add0(i)

    def add1(i):
        red1.add1(i)
        red2.add1(i)

    def finish(i):
        g_in[i] = red1.last(i)
        g_out[i] = red2.last(i)

    def when_layer(k, lag, *fns):
        @pl.when((k >= lag) & (k < layers + lag))
        def _():
            for fn in fns:
                fn(layers - 1 - (k - lag))

    send_cot = remote(gs.at[0], cot_in, zsem.at[0], zsem.at[1], to_z)
    send_dx1 = remote(dxs.at[1], dxs.at[1], zsem.at[2], zsem.at[3], to_z)
    send_dx0 = remote(gs.at[0], dxs.at[0], zsem.at[4], zsem.at[5], to_z)

    next_x = pltpu.make_async_copy(x_in.at[0, 0], dxs.at[0], asem.at[4])
    for lo, hi in ((0, 3), (3, layers)):
        for i in range(lo, hi):
            for cp in load(i):
                cp.wait()
        forward(lo, hi)
        if lo == 0:
            load_g.start()
            load_acc1.start()
            load_acc2.start()
            load_ids.start()
            load_emb(lambda cp: cp.start())
            pl.when(pp == 0)(next_x.start)
    load_acc1.wait()
    load_acc2.wait()
    load_g.wait()
    load_ids.wait()
    lane = lax.broadcasted_iota(jnp.int32, (128, 128), 1)
    for j in range(2):
        for b in range(tokens // 128):
            ids = ids_in[j:j + 1, b * 128:(b + 1) * 128].astype(F32)
            ids = jnp.broadcast_to(ids, (128, 128)).T.astype(jnp.int32)
            rel[pl.ds(j * tokens + b * 128, 128)] = ids - lane
    enter()

    @pl.when(pp == 1)
    def _():
        group = 3

        def blocks(k, carry):
            for n in range(group):
                block_backward(layers - 1 - k * group - n, True, True)
            for n in range(group):
                start0(layers - 1 - k * group - n)

            @pl.when(k >= 1)
            def _():
                for n in range(group):
                    add0(layers - 1 - (k - 1) * group - n)
                    start1(layers - 1 - (k - 1) * group - n)

            return carry

        lax.fori_loop(0, layers // group, blocks, 0)
        send_cot.start()
        for i in reversed(range(group)):
            add0(i)
            start1(i)

        def step(k, carry):
            when_layer(k, 0, add1, start2)
            when_layer(k, 3, finish)
            return carry

        lax.fori_loop(0, layers + 3, step, 0)
        send_dx1.wait_recv()
        dxt[:, pl.ds(tokens, tokens)] = dxs[1].T
        send_dx0.wait_recv()
        dxt[:, pl.ds(0, tokens)] = dxs[0].T

    @pl.when(pp == 0)
    def _():
        def back(k, carry):
            block_backward(layers - 1 - k, True, False)
            return carry

        lax.fori_loop(0, layers, back, 0, unroll=layers)
        dxs[1] = gs[0]
        send_dx1.start()
        next_x.wait()
        xs[0] = dxs[0]
        forward(0, layers)
        dxt[:, pl.ds(tokens, tokens)] = dxs[1].T
        send_cot.wait_recv()
        gs[layers % 2] = cot_in[...]

        for i in reversed(range(layers)):
            block_backward(i, False, True, send_dx0.start if i == 0 else None)
            start0(i)
            if i + 2 < layers:
                add0(i + 2)
                start1(i + 2)
        for i in (1, 0):
            add0(i)
            start1(i)
        dxt[:, pl.ds(0, tokens)] = gs[0].T

    load_emb(lambda cp: cp.wait())

    def own(red):
        return 4 * red.c + 2 * red.p + red.q

    def zcopy(i):
        return (remote(sa.at[i, own(reda)], za.at[i], fsem.at[0, i], fsem.at[1, i], to_z),
                remote(sb.at[i, own(redb)], zb.at[i], fsem.at[2, i], fsem.at[3, i], to_z))

    def build(i):
        for part, dst, slab in ((0, sa, slab_xy), (1, sb, slab_yx)):
            def piece(j, carry):
                at = pl.multiple_of(j * block, block)
                row = pl.multiple_of((2 * i + part) * width + j * block, block)
                base = my_row + row
                ids = rel[...]
                hot = jnp.concatenate([jnp.where(ids == base + 128 * n, 1.0, 0.0).astype(BF16) for n in range(block // 128)], axis=1)
                val = buf[pl.ds(row, block), :].T + dot(dxt[...], hot, 1, 0)
                val = val.astype(BF16)
                for d in range(8):
                    dst[i, slab(d), :, pl.ds(at, block)] = val[d * 16:(d + 1) * 16]
                return carry

            lax.fori_loop(0, width // block, piece, 0)

    def lanes(row, i, part):
        return pl.ds(pl.multiple_of(row + (2 * i + part) * width, 128), width)

    def emb_finish(i):
        for part, red in ((0, reda), (1, redb)):
            val = red.last(i).astype(BF16)
            red.src[i, own(red)] = val
            emb_out[:, lanes(my_row, i, part)] = val
        for cp in zcopy(i):
            cp.start()

    def put(i):
        for cp in zcopy(i):
            cp.wait_recv()
        emb_out[:, lanes(their_row, i, 0)] = za[i]
        emb_out[:, lanes(their_row, i, 1)] = zb[i]

    def emb_step(k, carry):
        def stage(lag, fn, count=mine):
            @pl.when((k >= lag) & (k < count + lag))
            def _():
                fn(k - lag)

        def late(lag, fn):
            for n in range(2):
                at = 2 * (k - lag) + n

                @pl.when((pp == 0) & (at >= 0) & (at < layers))
                def _():
                    fn(layers - 1 - at)

        stage(0, lambda i: (build(i), reda.copy0(i).start(), redb.copy0(i).start()))
        late(0, lambda i: (add1(i), start2(i)))
        stage(1, lambda i: (reda.add0(i), redb.add0(i), reda.copy1(i).start(), redb.copy1(i).start()))
        stage(3, lambda i: (reda.add1(i), redb.add1(i), reda.copy2(i).start(), redb.copy2(i).start()))
        stage(5, emb_finish)
        late(4, finish)
        stage(7, put, theirs)
        return carry

    lax.fori_loop(0, pairs + 8, emb_step, 0)

    @pl.when(pp == 1)
    def _():
        send_cot.wait_send()

    @pl.when(pp == 0)
    def _():
        send_dx1.wait_send()
        send_dx0.wait_send()

    def drain_layer(i, carry):
        red1.drain(i)
        red2.drain(i)
        return carry

    lax.fori_loop(0, layers, drain_layer, 0)

    def drain_pair(i, carry):
        @pl.when(i < mine)
        def _():
            reda.drain(i)
            redb.drain(i)
            for cp in zcopy(i):
                cp.wait_send()

        return carry

    lax.fori_loop(0, pairs, drain_pair, 0)


def fused(tok_ids, d_out, stored_x, w_in, w_out, acc_in, acc_out, acc_emb):
    layers, hid, ff = w_in.shape
    tokens = d_out.shape[1]
    vocab = acc_emb.shape[0]
    split, width = 9, 768
    pairs = pl.cdiv(vocab, 2 * width) - split
    half = 2 * pairs * width
    n1, n2 = hid // 8, ff // 8

    def side(count, *shape):
        return [pltpu.VMEM((count, 8, *shape), BF16), pltpu.VMEM((count, 4, *shape), BF16),
                pltpu.VMEM((count, 2, *shape), BF16), pltpu.VMEM((count, *shape), BF16)]

    piece = pltpu.VMEM((pairs, n1, width), BF16)
    return pl.pallas_call(
        functools.partial(fused_kernel, layers, pairs, split, width, vocab),
        out_shape=(pltpu.VMEM((layers, n1, ff), F32), pltpu.VMEM((layers, n2, hid), F32), pltpu.VMEM((n1, 2 * (pairs + split) * width), BF16)),
        in_specs=[ANY, ANY, ANY, ANY, ANY, ANY, ANY, ANY],
        out_specs=(VM, VM, VM),
        scratch_shapes=[
            pltpu.VMEM((layers, hid, ff), BF16),
            pltpu.VMEM((layers, ff, hid), BF16),
            pltpu.VMEM((layers + 1, tokens, hid), BF16),
            pltpu.VMEM((layers, tokens, ff), BF16),
            pltpu.VMEM((layers, tokens, ff), F32),
            pltpu.VMEM((2, tokens, hid), BF16),
            pltpu.VMEM((tokens, ff), BF16),
            pltpu.VMEM((layers, hid, ff), F32),
            pltpu.VMEM((layers, hid, ff), F32),
            pltpu.VMEM((layers, ff, hid), F32),
            pltpu.VMEM((tokens, hid), BF16),
            pltpu.VMEM((2, tokens, hid), BF16),
            *side(layers, n1, ff),
            *side(layers, n2, hid),
            pltpu.VMEM((2, tokens), jnp.int32),
            pltpu.VMEM((2 * tokens, 128), jnp.int32),
            pltpu.VMEM((half, hid), F32),
            pltpu.VMEM((hid, 2 * tokens), BF16),
            *side(pairs, n1, width),
            *side(pairs, n1, width),
            piece, piece,
            pltpu.SemaphoreType.DMA((2, layers)),
            pltpu.SemaphoreType.DMA((6,)),
            pltpu.SemaphoreType.DMA((6,)),
            pltpu.SemaphoreType.DMA((6, layers)),
            pltpu.SemaphoreType.DMA((6, layers)),
            pltpu.SemaphoreType.DMA,
            pltpu.SemaphoreType.DMA((6, pairs)),
            pltpu.SemaphoreType.DMA((6, pairs)),
            pltpu.SemaphoreType.DMA((4, pairs)),
        ],
        compiler_params=pltpu.CompilerParams(collective_id=0, has_side_effects=True, vmem_limit_bytes=65 * 10**6),
    )(tok_ids, d_out, stored_x, w_in, w_out, acc_in, acc_out, acc_emb)


def mean_kernel(a, b, e, g_in, g_out, g_emb):
    g_in[...] = a[...] * 0.125
    g_out[...] = b[...] * 0.125
    g_emb[...] = e[:, :g_emb.shape[1]].astype(F32) * 0.125


def mean(a, b, e, vocab):
    return pl.pallas_call(
        mean_kernel,
        out_shape=(jax.ShapeDtypeStruct(a.shape, F32), jax.ShapeDtypeStruct(b.shape, F32), jax.ShapeDtypeStruct((e.shape[0], vocab), F32)),
        in_specs=[VM, VM, VM],
        out_specs=(VM, VM, VM),
        compiler_params=pltpu.CompilerParams(vmem_limit_bytes=8 * 2**20),
    )(a, b, e)


def solution(mesh):
    def device_body(tok_ids, d_out, stored_x, w_in, w_out, acc_in, acc_out, acc_emb):
        vocab, hid = acc_emb.shape[1:]
        sums = fused(tok_ids, d_out, stored_x, w_in, w_out, acc_in, acc_out, acc_emb.reshape(vocab, 1, hid))
        grad_in, grad_out, grad_emb = mean(*sums, vocab)
        return grad_in, grad_out, grad_emb.T

    return jax.shard_map(
        device_body,
        mesh=mesh,
        in_specs=(P(None, "dp"), P("pp", "dp", None), P("pp", None, "dp", None), P("pp", None, None), P("pp", None, None),
                  P("pp", "dp", None, None), P("pp", "dp", None, None), P("dp", None, None)),
        out_specs=(P("pp", "dp", None), P("pp", "dp", None), P(None, "dp")),
        check_vma=False,
    )
```

```python
import functools

import jax
import jax.numpy as jnp
from jax import lax
from jax.experimental import pallas as pl
from jax.experimental.pallas import tpu as pltpu
from jax.sharding import PartitionSpec as P

MESH = pl.DeviceIdType.MESH
C0 = 0.7978845608028654
C1 = 0.044715
F32, BF16 = jnp.float32, jnp.bfloat16
ANY = pl.BlockSpec(memory_space=pl.ANY)
VM = pl.BlockSpec(memory_space=pltpu.VMEM)


def coords():
    pp, d = lax.axis_index("pp"), lax.axis_index("dp")
    y, x, c = d // 4, (d // 2) % 2, d % 2
    to_x = {"pp": pp, "dp": d + 2 - 4 * x}
    to_y = {"pp": pp, "dp": d + 4 - 8 * y}
    to_c = {"pp": pp, "dp": d + 1 - 2 * c}
    to_z = {"pp": 1 - pp, "dp": d}
    return pp, y, x, c, to_x, to_y, to_c, to_z


def knock(neighbours):
    barrier = pltpu.get_barrier_semaphore()
    for dev in neighbours:
        pl.semaphore_signal(barrier, inc=1, device_id=dev, device_id_type=MESH)
    return lambda: pl.semaphore_wait(barrier, len(neighbours))


def remote(src, dst, send, recv, dev):
    return pltpu.make_async_remote_copy(src_ref=src, dst_ref=dst, send_sem=send, recv_sem=recv, device_id=dev, device_id_type=MESH)


def slab_xy(d):
    return (d % 2) * 4 + ((d // 2) % 2) * 2 + d // 4


def slab_yx(d):
    return (d % 2) * 4 + (d // 4) * 2 + (d // 2) % 2


class Reduce:
    def __init__(self, src, r0, r1, r2, sems, to, c, p, q):
        self.src, self.r0, self.r1, self.r2, self.sems, self.to = src, r0, r1, r2, sems, to
        self.c, self.p, self.q = c, p, q

    def copy0(self, i):
        return remote(self.src.at[i, pl.ds(4 * (1 - self.c), 4)], self.r0.at[i], self.sems.at[0, i], self.sems.at[1, i], self.to[0])

    def copy1(self, i):
        at = 4 * self.c + 2 * (1 - self.p)
        return remote(self.src.at[i, pl.ds(at, 2)], self.r1.at[i], self.sems.at[2, i], self.sems.at[3, i], self.to[1])

    def copy2(self, i):
        at = 4 * self.c + 2 * self.p + 1 - self.q
        return remote(self.src.at[i, at], self.r2.at[i], self.sems.at[4, i], self.sems.at[5, i], self.to[2])

    def add0(self, i):
        self.copy0(i).wait_recv()
        for k in range(4):
            at = 4 * self.c + k
            self.src[i, at] = (self.src[i, at].astype(F32) + self.r0[i, k].astype(F32)).astype(BF16)

    def add1(self, i):
        self.copy1(i).wait_recv()
        for k in range(2):
            at = 4 * self.c + 2 * self.p + k
            self.src[i, at] = (self.src[i, at].astype(F32) + self.r1[i, k].astype(F32)).astype(BF16)

    def last(self, i):
        self.copy2(i).wait_recv()
        at = 4 * self.c + 2 * self.p + self.q
        return self.src[i, at].astype(F32) + self.r2[i].astype(F32)

    def drain(self, i):
        self.copy0(i).wait_send()
        self.copy1(i).wait_send()
        self.copy2(i).wait_send()


def dot(a, b, ca, cb):
    return lax.dot_general(a, b, (((ca,), (cb,)), ((), ())), preferred_element_type=F32)


def fused_kernel(layers, pairs, split, width, vocab, tok_ids, d_out, x_in, w_in, w_out, acc_in, acc_out, acc_emb, g_in, g_out, emb_out,
                 w1, w2, xs, hid, slope, gs, dh, dw1, dw2, acc2, cot_in, dxs, s1, s1a, s1b, s1c, s2, s2a, s2b, s2c,
                 ids_in, rel, buf, dxt, sa, sa0, sa1, sa2, sb, sb0, sb1, sb2, za, zb,
                 wsem, asem, zsem, sem1, sem2, esem, sema, semb, fsem):
    pp, y, x, c, to_x, to_y, to_c, to_z = coords()
    tokens = dxs.shape[1]
    head = 2 * split * width
    mine, theirs = split + pp * (pairs - split), pairs - pp * (pairs - split)
    my_row, their_row = pp * head, (1 - pp) * head
    block = width

    def load(i):
        return (pltpu.make_async_copy(w_in.at[i], w1.at[i], wsem.at[0, i]),
                pltpu.make_async_copy(w_out.at[i], w2.at[i], wsem.at[1, i]))

    def load_emb(act):
        def one(size, base):
            act(pltpu.make_async_copy(acc_emb.at[pl.ds(base, size), 0, :], buf.at[pl.ds(0, size)], esem))

        @pl.when(pp == 0)
        def _():
            one(head, 0)

        @pl.when(pp == 1)
        def _():
            one(vocab - head, head)

    load_x = pltpu.make_async_copy(x_in.at[0, 1 - pp], xs.at[0], asem.at[2])
    load_g = pltpu.make_async_copy(d_out.at[0], gs.at[layers % 2], asem.at[3])
    load_acc1 = pltpu.make_async_copy(acc_in.at[:, 0], dw1, asem.at[0])
    load_acc2 = pltpu.make_async_copy(acc_out.at[:, 0], acc2, asem.at[1])
    enter = knock((to_x, to_y, to_c, to_z))
    load_ids = pltpu.make_async_copy(tok_ids, ids_in, asem.at[5])
    load_x.start()
    for i in range(layers):
        for cp in load(i):
            cp.start()

    load_x.wait()

    red1 = Reduce(s1, s1a, s1b, s1c, sem1, (to_c, to_x, to_y), c, x, y)
    red2 = Reduce(s2, s2a, s2b, s2c, sem2, (to_c, to_y, to_x), c, y, x)
    reda = Reduce(sa, sa0, sa1, sa2, sema, (to_c, to_x, to_y), c, x, y)
    redb = Reduce(sb, sb0, sb1, sb2, semb, (to_c, to_y, to_x), c, y, x)

    def forward(lo, hi):
        def body(i, carry):
            xc = xs[i]
            h = dot(xc, w1[i], 1, 0).astype(BF16).astype(F32)
            h2 = h * h
            t = jnp.tanh(h * (C0 + (C0 * C1) * h2))
            cdf = 0.5 + 0.5 * t
            a = (h * cdf).astype(BF16)
            hid[i] = a
            slope[i] = cdf + h * ((cdf * (1.0 - cdf)) * (2.0 * C0 + (6.0 * C0 * C1) * h2))
            xs[i + 1] = (xc.astype(F32) + dot(a, w2[i], 1, 0)).astype(BF16)
            return carry

        lax.fori_loop(lo, hi, body, 0, unroll=hi - lo)

    def block_backward(i, first, final, then=None):
        gc = gs[(i + 1) % 2]
        da = dot(gc, w2[i], 1, 1).astype(BF16).astype(F32)
        dhc = (da * slope[i]).astype(BF16)
        dh[...] = dhc
        gs[i % 2] = (gc.astype(F32) + dot(dhc, w1[i], 1, 1)).astype(BF16)
        if then is not None:
            then()
        new2 = dot(gs[(i + 1) % 2], hid[i], 0, 0)
        if not first:
            new2 = new2 + dw2[i]
        new1 = dot(xs[i], dh[...], 0, 0) + dw1[i]
        if not final:
            dw1[i] = new1
            dw2[i] = new2
            return
        new1 = new1.astype(BF16)
        n1 = new1.shape[0] // 8
        for d in range(8):
            s1[i, slab_xy(d)] = new1[d * n1:(d + 1) * n1]
        new2 = (new2.T + acc2[i]).astype(BF16)
        n2 = new2.shape[0] // 8
        for d in range(8):
            s2[i, slab_yx(d)] = new2[d * n2:(d + 1) * n2]

    def start0(i):
        red1.copy0(i).start()
        red2.copy0(i).start()

    def start1(i):
        red1.copy1(i).start()
        red2.copy1(i).start()

    def start2(i):
        red1.copy2(i).start()
        red2.copy2(i).start()

    def add0(i):
        red1.add0(i)
        red2.add0(i)

    def add1(i):
        red1.add1(i)
        red2.add1(i)

    def finish(i):
        g_in[i] = red1.last(i)
        g_out[i] = red2.last(i)

    def when_layer(k, lag, *fns):
        @pl.when((k >= lag) & (k < layers + lag))
        def _():
            for fn in fns:
                fn(layers - 1 - (k - lag))

    send_cot = remote(gs.at[0], cot_in, zsem.at[0], zsem.at[1], to_z)
    send_dx1 = remote(dxs.at[1], dxs.at[1], zsem.at[2], zsem.at[3], to_z)
    send_dx0 = remote(gs.at[0], dxs.at[0], zsem.at[4], zsem.at[5], to_z)

    next_x = pltpu.make_async_copy(x_in.at[0, 0], dxs.at[0], asem.at[4])
    for lo, hi in ((0, 3), (3, layers)):
        for i in range(lo, hi):
            for cp in load(i):
                cp.wait()
        forward(lo, hi)
        if lo == 0:
            load_g.start()
            load_acc1.start()
            load_acc2.start()
            load_ids.start()
            load_emb(lambda cp: cp.start())
            pl.when(pp == 0)(next_x.start)
    load_acc1.wait()
    load_acc2.wait()
    load_g.wait()
    load_ids.wait()
    lane = lax.broadcasted_iota(jnp.int32, (128, 128), 1)
    for j in range(2):
        for b in range(tokens // 128):
            ids = ids_in[j:j + 1, b * 128:(b + 1) * 128].astype(F32)
            ids = jnp.broadcast_to(ids, (128, 128)).T.astype(jnp.int32)
            rel[pl.ds(j * tokens + b * 128, 128)] = ids - lane
    enter()

    @pl.when(pp == 1)
    def _():
        group = 3

        def blocks(k, carry):
            for n in range(group):
                block_backward(layers - 1 - k * group - n, True, True)
            for n in range(group):
                start0(layers - 1 - k * group - n)

            @pl.when(k >= 1)
            def _():
                for n in range(group):
                    add0(layers - 1 - (k - 1) * group - n)
                    start1(layers - 1 - (k - 1) * group - n)

            return carry

        lax.fori_loop(0, layers // group, blocks, 0)
        send_cot.start()
        for i in reversed(range(group)):
            add0(i)
            start1(i)

        def step(k, carry):
            when_layer(k, 0, add1, start2)
            when_layer(k, 3, finish)
            return carry

        lax.fori_loop(0, layers + 3, step, 0)
        send_dx1.wait_recv()
        dxt[:, pl.ds(tokens, tokens)] = dxs[1].T
        send_dx0.wait_recv()
        dxt[:, pl.ds(0, tokens)] = dxs[0].T

    @pl.when(pp == 0)
    def _():
        def back(k, carry):
            block_backward(layers - 1 - k, True, False)
            return carry

        lax.fori_loop(0, layers, back, 0, unroll=layers)
        dxs[1] = gs[0]
        send_dx1.start()
        next_x.wait()
        xs[0] = dxs[0]
        forward(0, layers)
        dxt[:, pl.ds(tokens, tokens)] = dxs[1].T
        send_cot.wait_recv()
        gs[layers % 2] = cot_in[...]

        for i in reversed(range(layers)):
            block_backward(i, False, True, send_dx0.start if i == 0 else None)
            start0(i)
            if i + 2 < layers:
                add0(i + 2)
                start1(i + 2)
        for i in (1, 0):
            add0(i)
            start1(i)
        dxt[:, pl.ds(0, tokens)] = gs[0].T

    load_emb(lambda cp: cp.wait())

    def own(red):
        return 4 * red.c + 2 * red.p + red.q

    def zcopy(i):
        return (remote(sa.at[i, own(reda)], za.at[i], fsem.at[0, i], fsem.at[1, i], to_z),
                remote(sb.at[i, own(redb)], zb.at[i], fsem.at[2, i], fsem.at[3, i], to_z))

    def build(i):
        for part, dst, slab in ((0, sa, slab_xy), (1, sb, slab_yx)):
            def piece(j, carry):
                at = pl.multiple_of(j * block, block)
                row = pl.multiple_of((2 * i + part) * width + j * block, block)
                base = my_row + row
                ids = rel[...]
                hot = jnp.concatenate([jnp.where(ids == base + 128 * n, 1.0, 0.0).astype(BF16) for n in range(block // 128)], axis=1)
                val = buf[pl.ds(row, block), :].T + dot(dxt[...], hot, 1, 0)
                val = val.astype(BF16)
                for d in range(8):
                    dst[i, slab(d), :, pl.ds(at, block)] = val[d * 16:(d + 1) * 16]
                return carry

            lax.fori_loop(0, width // block, piece, 0)

    def lanes(row, i, part):
        return pl.ds(pl.multiple_of(row + (2 * i + part) * width, 128), width)

    def emb_finish(i):
        for part, red in ((0, reda), (1, redb)):
            val = red.last(i).astype(BF16)
            red.src[i, own(red)] = val
            emb_out[:, lanes(my_row, i, part)] = val
        for cp in zcopy(i):
            cp.start()

    def put(i):
        for cp in zcopy(i):
            cp.wait_recv()
        emb_out[:, lanes(their_row, i, 0)] = za[i]
        emb_out[:, lanes(their_row, i, 1)] = zb[i]

    def emb_step(k, carry):
        def stage(lag, fn, count=mine):
            @pl.when((k >= lag) & (k < count + lag))
            def _():
                fn(k - lag)

        def late(lag, fn):
            for n in range(2):
                at = 2 * (k - lag) + n

                @pl.when((pp == 0) & (at >= 0) & (at < layers))
                def _():
                    fn(layers - 1 - at)

        stage(0, lambda i: (build(i), reda.copy0(i).start(), redb.copy0(i).start()))
        late(0, lambda i: (add1(i), start2(i)))
        stage(1, lambda i: (reda.add0(i), redb.add0(i), reda.copy1(i).start(), redb.copy1(i).start()))
        stage(3, lambda i: (reda.add1(i), redb.add1(i), reda.copy2(i).start(), redb.copy2(i).start()))
        stage(5, emb_finish)
        late(4, finish)
        stage(7, put, theirs)
        return carry

    lax.fori_loop(0, max(pairs, split) + 8, emb_step, 0)

    @pl.when(pp == 1)
    def _():
        send_cot.wait_send()

    @pl.when(pp == 0)
    def _():
        send_dx1.wait_send()
        send_dx0.wait_send()

    def drain_layer(i, carry):
        red1.drain(i)
        red2.drain(i)
        return carry

    lax.fori_loop(0, layers, drain_layer, 0)

    def drain_pair(i, carry):
        @pl.when(i < mine)
        def _():
            reda.drain(i)
            redb.drain(i)
            for cp in zcopy(i):
                cp.wait_send()

        return carry

    lax.fori_loop(0, max(pairs, split), drain_pair, 0)


def fused(tok_ids, d_out, stored_x, w_in, w_out, acc_in, acc_out, acc_emb):
    layers, hid, ff = w_in.shape
    tokens = d_out.shape[1]
    vocab = acc_emb.shape[0]
    split, width = 11, 768
    pairs = pl.cdiv(vocab, 2 * width) - split
    most = max(pairs, split)
    n1, n2 = hid // 8, ff // 8

    def side(count, *shape):
        return [pltpu.VMEM((count, 8, *shape), BF16), pltpu.VMEM((count, 4, *shape), BF16),
                pltpu.VMEM((count, 2, *shape), BF16), pltpu.VMEM((count, *shape), BF16)]

    piece = pltpu.VMEM((most, n1, width), BF16)
    return pl.pallas_call(
        functools.partial(fused_kernel, layers, pairs, split, width, vocab),
        out_shape=(pltpu.VMEM((layers, n1, ff), F32), pltpu.VMEM((layers, n2, hid), F32), pltpu.VMEM((n1, 2 * (pairs + split) * width), BF16)),
        in_specs=[ANY, ANY, ANY, ANY, ANY, ANY, ANY, ANY],
        out_specs=(VM, VM, VM),
        scratch_shapes=[
            pltpu.VMEM((layers, hid, ff), BF16),
            pltpu.VMEM((layers, ff, hid), BF16),
            pltpu.VMEM((layers + 1, tokens, hid), BF16),
            pltpu.VMEM((layers, tokens, ff), BF16),
            pltpu.VMEM((layers, tokens, ff), F32),
            pltpu.VMEM((2, tokens, hid), BF16),
            pltpu.VMEM((tokens, ff), BF16),
            pltpu.VMEM((layers, hid, ff), F32),
            pltpu.VMEM((layers, hid, ff), F32),
            pltpu.VMEM((layers, ff, hid), F32),
            pltpu.VMEM((tokens, hid), BF16),
            pltpu.VMEM((2, tokens, hid), BF16),
            *side(layers, n1, ff),
            *side(layers, n2, hid),
            pltpu.VMEM((2, tokens), jnp.int32),
            pltpu.VMEM((2 * tokens, 128), jnp.int32),
            pltpu.VMEM((2 * most * width, hid), F32),
            pltpu.VMEM((hid, 2 * tokens), BF16),
            *side(most, n1, width),
            *side(most, n1, width),
            piece, piece,
            pltpu.SemaphoreType.DMA((2, layers)),
            pltpu.SemaphoreType.DMA((6,)),
            pltpu.SemaphoreType.DMA((6,)),
            pltpu.SemaphoreType.DMA((6, layers)),
            pltpu.SemaphoreType.DMA((6, layers)),
            pltpu.SemaphoreType.DMA,
            pltpu.SemaphoreType.DMA((6, most)),
            pltpu.SemaphoreType.DMA((6, most)),
            pltpu.SemaphoreType.DMA((4, most)),
        ],
        compiler_params=pltpu.CompilerParams(collective_id=0, has_side_effects=True, vmem_limit_bytes=65 * 10**6),
    )(tok_ids, d_out, stored_x, w_in, w_out, acc_in, acc_out, acc_emb)


def mean_kernel(a, b, e, g_in, g_out, g_emb):
    g_in[...] = a[...] * 0.125
    g_out[...] = b[...] * 0.125
    g_emb[...] = e[:, :g_emb.shape[1]].astype(F32) * 0.125


def mean(a, b, e, vocab):
    return pl.pallas_call(
        mean_kernel,
        out_shape=(jax.ShapeDtypeStruct(a.shape, F32), jax.ShapeDtypeStruct(b.shape, F32), jax.ShapeDtypeStruct((e.shape[0], vocab), F32)),
        in_specs=[VM, VM, VM],
        out_specs=(VM, VM, VM),
        compiler_params=pltpu.CompilerParams(vmem_limit_bytes=8 * 2**20),
    )(a, b, e)


def solution(mesh):
    def device_body(tok_ids, d_out, stored_x, w_in, w_out, acc_in, acc_out, acc_emb):
        vocab, hid = acc_emb.shape[1:]
        sums = fused(tok_ids, d_out, stored_x, w_in, w_out, acc_in, acc_out, acc_emb.reshape(vocab, 1, hid))
        grad_in, grad_out, grad_emb = mean(*sums, vocab)
        return grad_in, grad_out, grad_emb.T

    return jax.shard_map(
        device_body,
        mesh=mesh,
        in_specs=(P(None, "dp"), P("pp", "dp", None), P("pp", None, "dp", None), P("pp", None, None), P("pp", None, None),
                  P("pp", "dp", None, None), P("pp", "dp", None, None), P("dp", None, None)),
        out_specs=(P("pp", "dp", None), P("pp", "dp", None), P(None, "dp")),
        check_vma=False,
    )
```
